256 devices in a mesh: grp: 4 (over y, x), det: 32 (over z), wlk: 2 (over core).
Axes of the slice: x: 2, y: 2, z: 32, core: 2. Of those that a mesh axis runs over, the one named last changes fastest.
The devices are a block of a 4x8x32 slice.
Arguments:
- greens: bfloat16 [256, 450, 150], P(('grp', 'det', 'wlk')), parts along dimension 0, may hold values from -2 to 2
- chol_vectors: bfloat16 [8192, 450, 150], P(('grp', 'det')), parts along dimension 0, may hold values from -0.0234375 to 0.0234375
- hole_orbitals: int32 [16384, 4], P(('grp', 'det')), parts along dimension 0, may hold values from 0 to 63, as said below
- particle_orbitals: int32 [16384, 4], P(('grp', 'det')), parts along dimension 0, may hold values from 0 to 63, as said below
- excitation_order: int32 [16384], P(('grp', 'det')), parts along dimension 0, may hold values from 0 to 4
- amplitudes: float32 [16384], P(('grp', 'det')), parts along dimension 0, may hold values from -0.6 to 0.6
Outputs:
- correlation: float32 [256], P(('grp', 'det', 'wlk')), parts along dimension 0
- force_bias: float32 [256, 2048], P(('grp', 'det', 'wlk')), parts along dimension 0
The draws below stay inside these ranges and needn't reach their ends.
There are 4 independent parts, one for each index of `grp`. The reference program is written for one: setup_inputs(seed, part) draws one part's arguments, and reference() takes and returns one part's arrays. A program takes and returns all parts, laid end to end along the dimension named above; each array names one. Nothing has to cross between parts.
Inputs may be any that keep to these rules, and one draw needn't show every extreme that they name: `hole_orbitals`: within each determinant the 4 entries are distinct. `particle_orbitals`: within each determinant the 4 entries are distinct.
All inputs are finite; a program needn't handle non-finite values.
Results may differ from the reference program's by a relative error of at most 0.00035.
Values may be sent and summed in bfloat16 or wider, within the bound.
A program may use at most 128 MiB of HBM per device.

```python
import jax
import jax.numpy as jnp
from jax import lax

NOCC = 150
NVIR = 450
NAO = 64
NAV = 64
MAXEXC = 4
WALKERS = 64
DETS = 4096
NCHOL = 2048


def distinct_picks(key, columns):
    scores = jax.random.randint(key, (DETS, columns), 0, 1 << 20) * columns + jnp.arange(columns)[None, :]
    return jnp.argsort(scores, axis=1)[:, :MAXEXC].astype(jnp.int32)


def draw_hole_orbitals(key, part):
    return distinct_picks(jax.random.fold_in(key, 11), NAO)


def draw_particle_orbitals(key, part):
    return distinct_picks(jax.random.fold_in(key, 23), NAV)


def draw_greens(key, part):
    first_key = jax.random.fold_in(jax.random.fold_in(key, 37), 0)
    virtual_rows = jnp.arange(NVIR)[:, None]
    occupied_columns = jnp.arange(NOCC)[None, :]
    in_active = (virtual_rows < NAV) & (occupied_columns >= NOCC - NAO)
    scale_map = jnp.where(in_active, 0.5, 0.02).astype(jnp.float32)
    values = jax.random.normal(first_key, (WALKERS, NVIR, NOCC), jnp.float32)
    return jnp.clip(values * scale_map[None, :, :], -2.0, 2.0).astype(jnp.bfloat16)


def set_ends(values, own_key, low, largest):
    shape = values.shape
    place = [jax.random.randint(jax.random.fold_in(own_key, axis), (), 0, shape[axis]) for axis in range(len(shape))]
    values = values.at[tuple(place)].set(low)
    longest = shape.index(max(shape))
    place[longest] = (place[longest] + 1) % shape[longest]
    return values.at[tuple(place)].set(largest)


def level_of(rng, dims, shards, low, high):
    factor_of, own = 1.0, jax.random.fold_in(rng, 6)
    for position, parts in shards:
        draws = jnp.exp(jax.random.uniform(jax.random.fold_in(own, position), (parts,), jnp.float32, low / len(shards), high / len(shards)))
        factor_of = factor_of * jnp.repeat(draws, dims[position] // parts).reshape([-1 if axis == position else 1 for axis in range(len(dims))])
    return factor_of


def normal_values(key, shape, scale, bound, cuts=(), kind=jnp.bfloat16):
    values = scale * jax.random.normal(key, shape, jnp.float32)
    if cuts:
        values = values * level_of(key, shape, cuts, -0.22, 0.18)
    return jnp.clip(values, -bound, bound).astype(kind)


def setup_inputs(seed: int = 0, part: int = 0) -> dict:
    key_list = jax.random.split(jax.random.key(seed), 7)
    own_keys = jax.random.split(jax.random.fold_in(key_list[6], part), 7)
    greens = draw_greens(jax.random.fold_in(jax.random.fold_in(key_list[6], part), 71), part)
    chol_vectors = normal_values(own_keys[1], (NCHOL, NVIR, NOCC), (NVIR * NOCC) ** -0.5, 0.0234375, ((0, 32),))
    hole_orbitals = draw_hole_orbitals(jax.random.fold_in(jax.random.fold_in(key_list[6], part), 71), part)
    particle_orbitals = draw_particle_orbitals(jax.random.fold_in(jax.random.fold_in(key_list[6], part), 71), part)
    excitation_order = set_ends(jax.random.randint(own_keys[4], (DETS,), 0, MAXEXC + 1), jax.random.fold_in(own_keys[4], 1), 0, MAXEXC).astype(jnp.int32)
    amplitudes = normal_values(own_keys[5], (DETS,), 0.1, 0.6, ((0, 32),), jnp.float32)
    return dict(greens=greens, chol_vectors=chol_vectors, hole_orbitals=hole_orbitals, particle_orbitals=particle_orbitals, excitation_order=excitation_order, amplitudes=amplitudes)


def minor_determinant(matrix):
    column_pairs = ((0, 1), (0, 2), (0, 3), (1, 2), (1, 3), (2, 3))
    parity = (1.0, -1.0, 1.0, 1.0, -1.0, 1.0)
    result = 0.0
    for number in range(6):
        first_column, second_column = column_pairs[number]
        third_column, fourth_column = column_pairs[5 - number]
        uppers = matrix[0][first_column] * matrix[1][second_column] - matrix[1][first_column] * matrix[0][second_column]
        lowers = matrix[2][third_column] * matrix[3][fourth_column] - matrix[3][third_column] * matrix[2][fourth_column]
        result = result + parity[number] * uppers * lowers
    return result

def divisor_below(amount, target):
    return max((candidate for candidate in range(1, min(target, amount) + 1) if amount % candidate == 0))

def reference(greens, chol_vectors, hole_orbitals, particle_orbitals, excitation_order, amplitudes):
    offset = NOCC - NAO
    walkers = greens.shape[0]
    active_green = greens[:, :NAV, offset:].astype(jnp.float32)
    det_count = hole_orbitals.shape[0]
    block_size = divisor_below(det_count, 1024)
    blocks = det_count // block_size

    def advance(totals, tables):
        hole_rows, particle_rows, order_rows, weight_rows = tables
        picked = active_green[:, particle_rows[:, :, None], hole_rows[:, None, :]]
        matrix = jnp.transpose(picked, (2, 3, 0, 1))
        positions = jnp.arange(MAXEXC)
        row_live = positions[:, None] < order_rows[None, :]
        live_mask = (row_live[:, None, :] & row_live[None, :, :])[:, :, None, :]
        identity = jnp.eye(MAXEXC, dtype=jnp.float32)[:, :, None, None]
        padded = jnp.where(live_mask, matrix, identity)
        ratios, pullback = jax.vjp(minor_determinant, padded)
        cofactors = pullback(jnp.ones_like(ratios))[0]
        weighted = jnp.where(live_mask, cofactors, 0.0) * weight_rows[None, None, None, :]
        correlation_part = lax.optimization_barrier(jnp.sum(ratios * weight_rows[None, :], axis=1))
        contrib = jnp.transpose(weighted, (2, 3, 0, 1))
        row_index = jnp.broadcast_to(particle_rows[:, :, None], (block_size, MAXEXC, MAXEXC))
        column_index = jnp.broadcast_to(hole_rows[:, None, :], (block_size, MAXEXC, MAXEXC))
        gradient = totals[0].at[:, row_index, column_index].add(contrib)
        return ((gradient, totals[1] + correlation_part), None)
    stacked = (hole_orbitals.reshape(blocks, block_size, MAXEXC), particle_orbitals.reshape(blocks, block_size, MAXEXC), excitation_order.reshape(blocks, block_size), amplitudes.reshape(blocks, block_size))
    zeros = (jnp.zeros((walkers, NAV, NAO), jnp.float32), jnp.zeros((walkers,), jnp.float32))
    (gradient, correlation_sum), _ = lax.scan(advance, zeros, stacked)
    correlation = 1.0 + correlation_sum
    gradient_rows = gradient.reshape(walkers, NAV * NAO).astype(jnp.bfloat16)
    vectors = chol_vectors.shape[0]
    flat_green = greens.reshape(walkers, NVIR * NOCC)
    flat_chol = chol_vectors.reshape(vectors, NVIR * NOCC)
    whole_term = lax.dot_general(flat_green, flat_chol, (((1,), (1,)), ((), ())), preferred_element_type=jnp.float32)
    active_chol = chol_vectors[:, :NAV, offset:].reshape(vectors, NAV * NAO)
    active_term = lax.dot_general(gradient_rows, active_chol, (((1,), (1,)), ((), ())), preferred_element_type=jnp.float32)
    force_bias = correlation[:, None] * whole_term + active_term
    return (correlation, force_bias)
```

```python
import functools

import jax
import jax.numpy as jnp
from jax import lax
from jax.experimental import pallas as pl
from jax.experimental.pallas import tpu as pltpu
from jax.sharding import PartitionSpec as P

NOCC = 150
NVIR = 450
NAO = 64
NAV = 64
MAXEXC = 4

MESH = pl.DeviceIdType.MESH
F32 = jnp.float32
BF16 = jnp.bfloat16

ROWS = 160
SENT = 152
LANES = 512
BLOCK = 16
BLOCKS = ROWS // BLOCK
BATCH = 4
CHUNKS = ((0, 32), (32, 32), (64, 32), (96, 32), (128, 24))
LAST_UP = (0, 1)
LAST_DOWN = (2, 3, 4)
STRIDE = 4
SHIFTS = (0, 1, 2, -1)


def minor_determinant(matrix):
    column_pairs = ((0, 1), (0, 2), (0, 3), (1, 2), (1, 3), (2, 3))
    parity = (1.0, -1.0, 1.0, 1.0, -1.0, 1.0)
    result = 0.0
    for number in range(6):
        first_column, second_column = column_pairs[number]
        third_column, fourth_column = column_pairs[5 - number]
        uppers = (
            matrix[0][first_column] * matrix[1][second_column]
            - matrix[1][first_column] * matrix[0][second_column]
        )
        lowers = (
            matrix[2][third_column] * matrix[3][fourth_column]
            - matrix[3][third_column] * matrix[2][fourth_column]
        )
        result = result + parity[number] * uppers * lowers
    return result


def transposed_dot(left, right):
    return lax.dot_general(left, right, (((1,), (1,)), ((), ())), preferred_element_type=F32)


def kernel(
    chips,
    schedule,
    green_ref,
    chol_ref,
    hole_ref,
    particle_ref,
    order_ref,
    amp_ref,
    corr_ref,
    bias_ref,
    raw_chol,
    chol,
    greens,
    total,
    tables,
    gradients,
    table_build,
    active,
    grad_total,
    corr_total,
    whole_rows,
    active_rows,
    message,
    inbox,
    chol_sem,
    ring_send,
    ring_recv,
    table_send,
    table_recv,
    table_send_near,
    table_recv_near,
    grad_send,
    grad_recv,
    grad_send_near,
    grad_recv_near,
    back_send,
    back_recv,
):
    half = chips // 2
    members = chips // STRIDE
    me = lax.axis_index("det")

    def chip(offset):
        return {"det": lax.rem(me + offset + chips, chips)}

    def chol_copy(block):
        start = block * BLOCK
        size = min(BLOCK, NOCC - start)
        return pltpu.make_async_copy(
            chol_ref.at[pl.ds(start, size)], raw_chol.at[pl.ds(start, size)], chol_sem.at[block]
        )

    for block in range(BLOCKS):
        chol_copy(block).start()

    barrier = pltpu.get_barrier_semaphore()
    partners = (1, -1, 2, -2, STRIDE, -STRIDE)
    for offset in partners:
        pl.semaphore_signal(barrier, inc=1, device_id=chip(offset), device_id_type=MESH)

    order = order_ref[...]
    live = lax.broadcasted_iota(jnp.int32, (MAXEXC, order.shape[1]), 0) < order
    table_build[...] = jnp.zeros_like(table_build)
    table_build[0:4, :] = jnp.where(live, hole_ref[...], -1).astype(F32)
    table_build[4:8, :] = jnp.where(live, particle_ref[...], -1).astype(F32)
    amp = amp_ref[...]
    high = amp.astype(BF16).astype(F32)
    middle = (amp - high).astype(BF16).astype(F32)
    table_build[8:9, :] = high
    table_build[9:10, :] = middle
    table_build[10:11, :] = amp - high - middle
    tables[0, 0] = table_build[...].astype(BF16)

    greens[0] = jnp.zeros((ROWS, LANES), BF16)
    greens[0, 0:NOCC, 0:NVIR] = green_ref[...]

    pl.semaphore_wait(barrier, len(partners))

    def hop_copy(buffer, send, recv, up, number):
        source = (number - 1) if up else (members - (number - 1)) % members
        target = number if up else members - number
        return pltpu.make_async_remote_copy(
            src_ref=buffer.at[0, source],
            dst_ref=buffer.at[0, target],
            send_sem=send.at[target],
            recv_sem=recv.at[target],
            device_id=chip(STRIDE if up else -STRIDE),
            device_id_type=MESH,
        )

    def near_copy(buffer, send, recv, place, member):
        return pltpu.make_async_remote_copy(
            src_ref=buffer.at[0, member],
            dst_ref=buffer.at[place, member],
            send_sem=send.at[place, member],
            recv_sem=recv.at[place, member],
            device_id=chip(SHIFTS[place]),
            device_id_type=MESH,
        )

    up_hops = members // 2
    down_hops = members - 1 - up_hops

    def start_spread(buffer, sems):
        send, recv, send_near, recv_near = sems
        hop_copy(buffer, send, recv, True, 1).start()
        if down_hops:
            hop_copy(buffer, send, recv, False, 1).start()
        for place in (1, 2, 3):
            near_copy(buffer, send_near, recv_near, place, 0).start()

    def hop_members(number):
        found = [number] if number <= up_hops else []
        return found + ([members - number] if number <= down_hops else [])

    def take_hop(buffer, sems, number):
        send, recv, send_near, recv_near = sems
        if number <= up_hops:
            hop_copy(buffer, send, recv, True, number).wait_recv()
            if number < up_hops:
                hop_copy(buffer, send, recv, True, number + 1).start()
        if number <= down_hops:
            hop_copy(buffer, send, recv, False, number).wait_recv()
            if number < down_hops:
                hop_copy(buffer, send, recv, False, number + 1).start()
        for member in hop_members(number):
            for place in (1, 2, 3):
                near_copy(buffer, send_near, recv_near, place, member).start()

    def take_near(buffer, sems, member):
        for place in (1, 2, 3):
            near_copy(buffer, sems[2], sems[3], place, member).wait_recv()

    def end_spread(buffer, sems):
        send, recv, send_near, recv_near = sems
        for number in range(1, up_hops + 1):
            hop_copy(buffer, send, recv, True, number).wait_send()
        for number in range(1, down_hops + 1):
            hop_copy(buffer, send, recv, False, number).wait_send()
        for member in range(members):
            for place in (1, 2, 3):
                near_copy(buffer, send_near, recv_near, place, member).wait_send()

    table_sems = (table_send, table_recv, table_send_near, table_recv_near)
    grad_sems = (grad_send, grad_recv, grad_send_near, grad_recv_near)

    def ring_copy(up, step, part):
        start, size = CHUNKS[part]
        if up:
            source, target = step - 1, step
        elif isinstance(step, int):
            source = half + step - 1 if step > 1 else 0
            target = half + step if step < half else half
        else:
            source, target = half + step - 1, half + step
        return pltpu.make_async_remote_copy(
            src_ref=greens.at[source, pl.ds(start, size)],
            dst_ref=greens.at[target, pl.ds(start, size)],
            send_sem=ring_send.at[0 if up else 1, step, part],
            recv_sem=ring_recv.at[0 if up else 1, step, part],
            device_id=chip(1 if up else -1),
            device_id_type=MESH,
        )

    start_spread(tables, table_sems)
    for part in range(len(CHUNKS)):
        ring_copy(True, 1, part).start()
        ring_copy(False, 1, part).start()

    total[...] = jnp.zeros_like(total)
    grad_total[...] = jnp.zeros_like(grad_total)
    corr_total[...] = jnp.zeros_like(corr_total)
    whole_rows[...] = jnp.zeros_like(whole_rows)
    active_rows[...] = jnp.zeros_like(active_rows)

    @pl.loop(1, chips)
    def _(slot):
        greens[slot, SENT:ROWS, :] = jnp.zeros((ROWS - SENT, LANES), BF16)

    shift_rows = lax.broadcasted_iota(jnp.int32, (NAO, ROWS // 2), 0)
    shift_columns = lax.broadcasted_iota(jnp.int32, (NAO, ROWS // 2), 1)
    offset = NOCC - NAO - ROWS // 2
    shift = (shift_columns == shift_rows + offset).astype(F32).astype(BF16)
    active[...] = lax.dot_general(
        shift,
        greens[0, ROWS // 2 : ROWS, 0:128],
        (((1,), (0,)), ((), ())),
        preferred_element_type=F32,
    ).astype(BF16)

    def clean_block(block, static_block):
        start = static_block * BLOCK
        size = min(BLOCK, NOCC - start)
        chol_copy(static_block).wait()
        if size < BLOCK:
            chol[pl.ds(start + size, BLOCK - size)] = jnp.zeros(
                (BLOCK - size, chol.shape[1], LANES), BF16
            )
        full = NVIR // 128 * 128
        chol[pl.ds(start, size), :, 0:full] = raw_chol[pl.ds(start, size), :, 0:full]
        chol[pl.ds(start, size), :, full:LANES] = jnp.zeros(
            (size, chol.shape[1], LANES - full), BF16
        )
        chol[pl.ds(start, size), :, full:NVIR] = raw_chol[pl.ds(start, size), :, full:NVIR]

    vectors = chol.shape[1]

    def add_block(slots, block):
        rows = pl.ds(pl.multiple_of(block * BLOCK, BLOCK), BLOCK)
        left = chol[rows].reshape(BLOCK * vectors, LANES)
        right = jnp.concatenate([greens[slot, rows, :] for slot in slots], axis=0)
        total[...] += transposed_dot(left, right)

    def take_total():
        columns = lax.broadcasted_iota(jnp.int32, (vectors, BATCH * BLOCK), 1)
        kept = jnp.zeros((vectors, BATCH * BLOCK), F32)
        for row in range(BLOCK):
            part = total[pl.ds(row * vectors, vectors), :]
            kept = kept + jnp.where(lax.rem(columns, BLOCK) == row, part, 0.0)
        total[...] = jnp.zeros_like(total)
        turned = kept.T
        return [
            jnp.sum(turned[number * BLOCK : (number + 1) * BLOCK, :], axis=0, keepdims=True)
            for number in range(BATCH)
        ]

    def keep_whole(slots, places):
        del slots
        for place, row in zip(places, take_total()):
            whole_rows[place, :, 0:vectors] = row

    def add_determinants(member):
        table = jnp.concatenate([tables[place, member] for place in range(4)], axis=1).astype(F32)
        width = table.shape[1]
        amplitude = table[8:9] + table[9:10] + table[10:11]
        orbital = lax.broadcasted_iota(jnp.int32, (NAO, width), 0).astype(F32)
        particle_hot = jnp.concatenate(
            [
                jnp.where(orbital == table[4 + row : 5 + row], 1.0, 0.0).astype(BF16)
                for row in range(MAXEXC)
            ],
            axis=1,
        )
        picked = jnp.dot(active[:, 0:NAV], particle_hot, preferred_element_type=F32)
        masks = [orbital == table[column : column + 1] for column in range(MAXEXC)]
        matrix = []
        for row in range(MAXEXC):
            own = picked[:, row * width : (row + 1) * width]
            entries = [
                jnp.sum(jnp.where(masks[column], own, 0.0), axis=0, keepdims=True)
                for column in range(MAXEXC)
            ]
            entries[row] = jnp.where(table[4 + row : 5 + row] < 0.0, 1.0, entries[row])
            matrix.append(entries)
        ratios, pullback = jax.vjp(minor_determinant, matrix)
        cofactors = pullback(jnp.ones_like(ratios))[0]
        corr_total[...] += ratios * amplitude
        uppers, lowers = [], []
        for row in range(MAXEXC):
            spread = jnp.zeros((NAO, width), F32)
            for column in range(MAXEXC):
                spread = jnp.where(masks[column], cofactors[row][column] * amplitude, spread)
            upper = spread.astype(BF16)
            uppers.append(upper)
            lowers.append((spread - upper.astype(F32)).astype(BF16))
        spread_all = jnp.concatenate(
            [jnp.concatenate(uppers, axis=1), jnp.concatenate(lowers, axis=1)], axis=0
        )
        grad_total[:, 0:NAV] += transposed_dot(spread_all, particle_hot)

    def finish_gradient():
        whole = grad_total[0:NAO, :] + grad_total[NAO : 2 * NAO, :]
        packed = whole[0 : NAO // 2] + pltpu.roll(whole[NAO // 2 : NAO], NAV, 1)
        gradients[0, 0] = packed.astype(BF16)

    def add_active(member):
        lanes = lax.broadcasted_iota(jnp.int32, (NAO // 2, 128), 1)
        unpacked = []
        for place in range(4):
            packed = gradients[place, member].astype(F32)
            unpacked.append(
                (
                    jnp.where(lanes < NAV, packed, 0.0).astype(BF16),
                    jnp.where(lanes < NAV, pltpu.roll(packed, NAV, 1), 0.0).astype(BF16),
                )
            )
        for block in range(NAO // BLOCK):
            start = NOCC - NAO + block * BLOCK
            left = chol[pl.ds(start, BLOCK), :, 0:128].reshape(BLOCK * vectors, 128)
            side, inner = divmod(block * BLOCK, NAO // 2)
            right = jnp.concatenate(
                [unpacked[place][side][inner : inner + BLOCK] for place in range(4)], axis=0
            )
            total[...] += transposed_dot(left, right)
        for place, row in enumerate(take_total()):
            index = (SHIFTS[place] + STRIDE * member) % chips
            active_rows[index, :, 0:vectors] = row

    events = {}
    for step, action in schedule:
        events.setdefault(step, []).append(action)

    def run_event(action):
        kind, number = action
        if kind == "table_hop":
            take_hop(tables, table_sems, number)
        elif kind == "determinants":
            take_near(tables, table_sems, number)
            add_determinants(number)
        elif kind == "gradient":
            finish_gradient()
            start_spread(gradients, grad_sems)
        elif kind == "grad_hop":
            take_hop(gradients, grad_sems, number)

    def forward(step, part, up, down):
        ring_copy(True, step, part).wait_recv()
        if up:
            ring_copy(True, step + 1, part).start()
        ring_copy(False, step, part).wait_recv()
        if down:
            ring_copy(False, step + 1, part).start()

    for step in (1, 2):
        for part in range(len(CHUNKS)):
            forward(step, part, True, True)
            block = (step - 1) * len(CHUNKS) + part
            clean_block(block, block)
        for action in events.get(step, ()):
            run_event(action)

    @pl.loop(3, half - 1)
    def _(step):
        pair = lax.div(step - 1, 2)
        second = lax.rem(step - 1, 2)
        places = (2 * pair - 1, 2 * pair, half + 2 * pair - 1, half + 2 * pair)
        for part in range(len(CHUNKS)):
            forward(step, part, True, True)
            add_block(places, second * len(CHUNKS) + part)

        @pl.when(second == 1)
        def _():
            keep_whole(places, (places[0], places[1], chips + 1 - 2 * pair, chips - 2 * pair))

        for when, actions in events.items():
            if 3 <= when < half - 1:

                @pl.when(step == when)
                def _(actions=actions):
                    for action in actions:
                        run_event(action)

    step = half - 1
    places = (half - 3, half - 2, 2 * half - 3, 2 * half - 2)
    for part in range(len(CHUNKS)):
        forward(step, part, part in LAST_UP, part in LAST_DOWN)
        for block in (2 * part, 2 * part + 1):
            add_block(places, block)
    keep_whole(places, (half - 3, half - 2, half + 3, half + 2))
    for action in events.get(step, ()):
        run_event(action)

    for member in range(members):
        if member != members // 2:
            if member:
                pass
            take_near(gradients, grad_sems, member)
            add_active(member)
    take_near(gradients, grad_sems, members // 2)
    add_active(members // 2)

    places = (half - 1, 2 * half - 1, half, 0)
    for part in range(len(CHUNKS)):
        if part in LAST_UP:
            ring_copy(True, half, part).wait_recv()
        else:
            ring_copy(False, half, part).wait_recv()
        for block in (2 * part, 2 * part + 1):
            add_block(places, block)
    keep_whole(places, (half - 1, half + 1, half, 0))

    message[...] = whole_rows[...] + pltpu.roll(active_rows[...], vectors, 2)

    def back_copy(offset):
        return pltpu.make_async_remote_copy(
            src_ref=message.at[offset],
            dst_ref=inbox.at[lax.rem(me, 2), lax.div(me, 2)],
            send_sem=back_send.at[offset],
            recv_sem=back_recv.at[offset],
            device_id={"det": lax.rem(me - offset + chips, chips)},
            device_id_type=MESH,
        )

    for offset in range(chips // 2, chips):
        back_copy(offset).start()
        if 0 < chips - offset < chips // 2:
            back_copy(chips - offset).start()
    inbox[lax.rem(me, 2), lax.div(me, 2)] = message[0]

    corr = 1.0 + jnp.sum(corr_total[...], axis=1, keepdims=True)
    corr_ref[...] = jnp.broadcast_to(corr, corr_ref.shape)

    end_spread(tables, table_sems)
    end_spread(gradients, grad_sems)

    for part in range(len(CHUNKS)):
        ring_copy(True, 1, part).wait_send()
        ring_copy(False, 1, part).wait_send()

    @pl.loop(2, half)
    def _(step):
        for part in range(len(CHUNKS)):
            ring_copy(True, step, part).wait_send()
            ring_copy(False, step, part).wait_send()

    for part in LAST_UP:
        ring_copy(True, half, part).wait_send()
    for part in LAST_DOWN:
        ring_copy(False, half, part).wait_send()

    for offset in range(1, chips):
        back_copy(offset).wait_send()

    def back_wait(offset):
        sender = lax.rem(me + offset, chips)
        pltpu.make_async_remote_copy(
            src_ref=message.at[offset],
            dst_ref=inbox.at[lax.rem(sender, 2), lax.div(sender, 2)],
            send_sem=back_send.at[offset],
            recv_sem=back_recv.at[offset],
            device_id=chip(offset),
            device_id_type=MESH,
        ).wait_recv()

    for offset in range(1, chips):
        back_wait(offset)

    even = inbox[0].reshape(chips // 2, 128)
    odd = inbox[1].reshape(chips // 2, 128)
    lanes = lax.broadcasted_iota(jnp.int32, even.shape, 1)
    even = corr * even + pltpu.roll(even, vectors, 1)
    odd = corr * pltpu.roll(odd, vectors, 1) + odd
    bias_ref[...] = jnp.where(lanes < vectors, even, odd)


def plan(chips):
    return (
        (2, ("table_hop", 1)),
        (3, ("determinants", 0)),
        (3, ("table_hop", 2)),
        (4, ("determinants", 1)),
        (4, ("determinants", 7)),
        (5, ("table_hop", 3)),
        (6, ("determinants", 2)),
        (6, ("determinants", 6)),
        (6, ("table_hop", 4)),
        (7, ("determinants", 3)),
        (7, ("determinants", 5)),
        (8, ("determinants", 4)),
        (8, ("gradient", 0)),
        (10, ("grad_hop", 1)),
        (12, ("grad_hop", 2)),
        (13, ("grad_hop", 3)),
        (15, ("grad_hop", 4)),
    )


def shards(greens, chol_vectors, hole_orbitals, particle_orbitals, excitation_order, amplitudes):
    chips = lax.axis_size("det")
    vectors = chol_vectors.shape[0]
    dets = hole_orbitals.shape[0]
    members = chips // STRIDE
    half = chips // 2
    dma = pltpu.SemaphoreType.DMA
    vmem = pl.BlockSpec(memory_space=pltpu.VMEM)
    corr, bias = pl.pallas_call(
        functools.partial(kernel, chips, plan(chips)),
        out_shape=(
            jax.ShapeDtypeStruct((1, 128), F32),
            jax.ShapeDtypeStruct((chips * vectors // 128, 128), F32),
        ),
        in_specs=[vmem, pl.BlockSpec(memory_space=pl.ANY), vmem, vmem, vmem, vmem],
        out_specs=(vmem, vmem),
        scratch_shapes=[
            pltpu.VMEM((NOCC, vectors, NVIR), BF16),
            pltpu.VMEM((ROWS, vectors, LANES), BF16),
            pltpu.VMEM((chips, ROWS, LANES), BF16),
            pltpu.VMEM((BLOCK * vectors, BATCH * BLOCK), F32),
            pltpu.VMEM((4, members, 16, dets), BF16),
            pltpu.VMEM((4, members, NAO // 2, 128), BF16),
            pltpu.VMEM((16, dets), F32),
            pltpu.VMEM((NAO, 128), BF16),
            pltpu.VMEM((2 * NAO, 128), F32),
            pltpu.VMEM((1, 4 * dets), F32),
            pltpu.VMEM((chips, 1, 128), F32),
            pltpu.VMEM((chips, 1, 128), F32),
            pltpu.VMEM((chips, 1, 128), F32),
            pltpu.VMEM((2, half, 1, 128), F32),
            dma((BLOCKS,)),
            dma((2, half + 1, len(CHUNKS))),
            dma((2, half + 1, len(CHUNKS))),
            dma((members,)),
            dma((members,)),
            dma((4, members)),
            dma((4, members)),
            dma((members,)),
            dma((members,)),
            dma((4, members)),
            dma((4, members)),
            dma((chips,)),
            dma((chips,)),
        ],
        compiler_params=pltpu.CompilerParams(
            collective_id=0, has_side_effects=True, vmem_limit_bytes=56 * 1024 * 1024
        ),
        name="walker_ring",
    )(
        jnp.transpose(greens, (0, 2, 1)).reshape(NOCC, NVIR),
        jnp.transpose(chol_vectors, (2, 0, 1)),
        jnp.transpose(hole_orbitals),
        jnp.transpose(particle_orbitals),
        excitation_order.reshape(1, dets),
        amplitudes.reshape(1, dets),
    )
    return (corr[0, 0:1], bias.reshape(1, chips * vectors))


def solution(mesh):
    placed = (
        P(("grp", "det", "wlk"), None, None),
        P(("grp", "det"), None, None),
        P(("grp", "det"), None),
        P(("grp", "det"), None),
        P(("grp", "det")),
        P(("grp", "det")),
    )
    return jax.shard_map(
        shards,
        mesh=mesh,
        in_specs=placed,
        out_specs=(P(("grp", "det", "wlk")), P(("grp", "det", "wlk"), None)),
        check_vma=False,
    )
```

```python
import functools

import jax
import jax.numpy as jnp
from jax import lax
from jax.experimental import pallas as pl
from jax.experimental.pallas import tpu as pltpu
from jax.sharding import PartitionSpec as P

NOCC = 150
NVIR = 450
NAO = 64
NAV = 64
MAXEXC = 4

MESH = pl.DeviceIdType.MESH
F32 = jnp.float32
BF16 = jnp.bfloat16

ROWS = 160
SENT = 152
LANES = 512
BLOCK = 16
BLOCKS = ROWS // BLOCK
BATCH = 8
FULL = NVIR // 128 * 128
PART = 64
SPARE = NOCC - ROWS // 2
LAST = (NVIR - FULL - PART, -(-NOCC // PART))
CHUNKS = (
    (1, 80, 72, 384),
    (0, 80, 72, 384),
    (1, 0, 48, 512),
    (0, 0, 48, 512),
    (1, 48, 32, 512),
    (0, 48, 32, 512),
)
LAST_UP = (0, 2, 4)
LAST_DOWN = (1, 3, 5)
CLEANED = {(1, 1): 0, (1, 2): 1, (1, 4): 2, (2, 0): 3, (2, 2): 4}
HALF_BLOCKS = ((0,), (1,), (2,), (3,), (4,), ())
ALL_BLOCKS = ((0, 1), (2,), (3, 4), (5,), (6, 7), (8, 9))
LAST_BLOCKS = ((), (5, 6, 7, 8, 9), (), (0, 1, 2), (), (3, 4))
STRIDE = 4
SHIFTS = (0, 1, 2, -1)


def minor_determinant(matrix):
    column_pairs = ((0, 1), (0, 2), (0, 3), (1, 2), (1, 3), (2, 3))
    parity = (1.0, -1.0, 1.0, 1.0, -1.0, 1.0)
    result = 0.0
    for number in range(6):
        first_column, second_column = column_pairs[number]
        third_column, fourth_column = column_pairs[5 - number]
        uppers = (
            matrix[0][first_column] * matrix[1][second_column]
            - matrix[1][first_column] * matrix[0][second_column]
        )
        lowers = (
            matrix[2][third_column] * matrix[3][fourth_column]
            - matrix[3][third_column] * matrix[2][fourth_column]
        )
        result = result + parity[number] * uppers * lowers
    return result


def transposed_dot(left, right):
    return lax.dot_general(left, right, (((1,), (1,)), ((), ())), preferred_element_type=F32)


def kernel(
    chips,
    green_ref,
    chol_ref,
    hole_ref,
    particle_ref,
    order_ref,
    amp_ref,
    corr_ref,
    bias_ref,
    raw_chol,
    chol,
    active_chol,
    greens,
    total,
    tables,
    gradients,
    table_build,
    peer_rows,
    active,
    grad_total,
    corr_total,
    message,
    inbox,
    peer_inbox,
    corr_out,
    corr_in,
    pack,
    leftover,
    chol_sem,
    swap_send,
    swap_recv,
    ring_send,
    ring_recv,
    table_send,
    table_recv,
    table_send_near,
    table_recv_near,
    grad_send,
    grad_recv,
    grad_send_near,
    grad_recv_near,
    back_send,
    back_recv,
):
    half = chips // 2
    members = chips // STRIDE
    vectors = chol.shape[1]
    me = lax.axis_index("det")
    core = lax.axis_index("wlk")
    barrier = pltpu.get_barrier_semaphore()

    def chip(offset):
        return {"det": lax.rem(me + offset + chips, chips)}

    def greet(offsets, other):
        for offset in offsets:
            pl.semaphore_signal(barrier, inc=1, device_id=chip(offset), device_id_type=MESH)
        pl.semaphore_signal(barrier, inc=1, device_id={"wlk": other}, device_id_type=MESH)

    def swap_copy(source, target, number, other):
        return pltpu.make_async_remote_copy(
            src_ref=source,
            dst_ref=target,
            send_sem=swap_send.at[number],
            recv_sem=swap_recv.at[number],
            device_id={"wlk": other},
            device_id_type=MESH,
        )

    def block_to_upper(part):
        _, start, size, lanes = CHUNKS[part]
        block = greens.at[0, 0, pl.ds(start, size), pl.ds(0, lanes)]
        return swap_copy(block, block, 4 + part // 2, 1)

    def rows_to_lower():
        rows = greens.at[0, 1, pl.ds(ROWS // 2, ROWS // 2), pl.ds(0, 128)]
        return swap_copy(rows, peer_rows, 1, 0)

    def inbox_swap(other):
        return swap_copy(inbox, peer_inbox, 2, other)

    def corr_to_upper():
        return swap_copy(corr_out, corr_in, 3, 1)

    def back_copy(offset):
        return pltpu.make_async_remote_copy(
            src_ref=message.at[offset],
            dst_ref=inbox.at[lax.rem(me, 2), lax.div(me, 2)],
            send_sem=back_send.at[offset],
            recv_sem=back_recv.at[offset],
            device_id={"det": lax.rem(me - offset + chips, chips)},
            device_id_type=MESH,
        )

    def back_wait(offset):
        sender = lax.rem(me + offset, chips)
        pltpu.make_async_remote_copy(
            src_ref=message.at[offset],
            dst_ref=inbox.at[lax.rem(sender, 2), lax.div(sender, 2)],
            send_sem=back_send.at[offset],
            recv_sem=back_recv.at[offset],
            device_id=chip(offset),
            device_id_type=MESH,
        ).wait_recv()

    def take_total():
        columns = lax.broadcasted_iota(jnp.int32, (vectors, BATCH * BLOCK), 1)
        kept = jnp.zeros((vectors, BATCH * BLOCK), F32)
        for row in range(BLOCK):
            part = total[pl.ds(row * vectors, vectors), :]
            kept = kept + jnp.where(lax.rem(columns, BLOCK) == row, part, 0.0)
        total[...] = jnp.zeros_like(total)
        turned = kept.T
        return [
            jnp.sum(turned[number * BLOCK : (number + 1) * BLOCK, :], axis=0, keepdims=True)
            for number in range(BATCH)
        ]

    def keep_rows(places):
        rows = take_total()
        for number, place in enumerate(places):
            message[place] = jnp.concatenate([rows[2 * number], rows[2 * number + 1]], axis=1)

    def own_walker(index):
        greens[0, index] = jnp.zeros((ROWS, LANES), BF16)
        greens[0, index, 0:NOCC, 0:NVIR] = green_ref[...]
        tile = greens[0, index, :, FULL:LANES].astype(F32)
        middle = ROWS // 2
        lanes = lax.broadcasted_iota(jnp.int32, tile.shape, 1)
        rows = lax.broadcasted_iota(jnp.int32, tile.shape, 0)
        further = pltpu.roll(tile[middle:], PART, 1)
        packed = jnp.where(lanes[:middle] < PART, tile[:middle], further)
        for column in range(LAST[0]):
            for third in range(LAST[1]):
                match = (lanes == rows + (1 - third) * PART) & (lanes >= PART)
                row = jnp.sum(
                    jnp.where(match, tile[:, PART + column : PART + column + 1], 0.0),
                    axis=0,
                    keepdims=True,
                )
                place = SPARE + LAST[1] * column + third
                packed = jnp.where(
                    (rows[:middle] == place) & (lanes[:middle] >= PART), row, packed
                )
        greens[0, index, 0:middle, FULL:LANES] = packed.astype(BF16)
        greens[0, index, middle:ROWS, FULL:LANES] = jnp.zeros((middle, LANES - FULL), BF16)

    def write_bias(corr, whole, term, upper):
        even = corr * whole[0].reshape(half, 128) + term[0].reshape(half, 128)
        odd = corr * whole[1].reshape(half, 128) + term[1].reshape(half, 128)
        lanes = lax.broadcasted_iota(jnp.int32, even.shape, 1)
        if upper:
            even = pltpu.roll(even, vectors, 1)
        else:
            odd = pltpu.roll(odd, vectors, 1)
        bias_ref[...] = jnp.where(lanes < vectors, even, odd)
        corr_ref[...] = jnp.broadcast_to(corr, corr_ref.shape)

    def ring_copy(up, step, part):
        walker, start, size, lanes = CHUNKS[part]
        if up:
            source, target = step - 1, step
        elif isinstance(step, int):
            source = half + step - 1 if step > 1 else 0
            target = half + step if step < half else half
        else:
            source, target = half + step - 1, half + step
        return pltpu.make_async_remote_copy(
            src_ref=greens.at[source, walker, pl.ds(start, size), pl.ds(0, lanes)],
            dst_ref=greens.at[target, walker, pl.ds(start, size), pl.ds(0, lanes)],
            send_sem=ring_send.at[0 if up else 1, step, part],
            recv_sem=ring_recv.at[0 if up else 1, step, part],
            device_id=chip(1 if up else -1),
            device_id_type=MESH,
        )

    def chol_copy(block):
        start = block * BLOCK
        size = min(BLOCK, NOCC - start)
        return pltpu.make_async_copy(
            chol_ref.at[pl.ds(start, size)], raw_chol.at[pl.ds(start, size)], chol_sem.at[block]
        )

    def packing():
        rows = lax.broadcasted_iota(jnp.int32, pack.shape, 0)
        columns = lax.broadcasted_iota(jnp.int32, pack.shape, 1)
        within = lax.rem(columns, 128)
        last = PART + jnp.where(within < PART, 1, 0)
        source = jnp.where(
            columns < 128,
            jnp.where(columns < PART, columns, columns + 128 - PART),
            jnp.where(columns < 256, last, last + 128),
        )
        pack[...] = jnp.where(rows == source, 1.0, 0.0).astype(BF16)

    def clean_pair(pair):
        low = pair * BLOCK
        high = ROWS // 2 + low
        size = min(BLOCK, NOCC - high)
        chol_copy(pair).wait()
        chol_copy(pair + BLOCKS // 2).wait()
        tiles = []
        for start, count in ((low, BLOCK), (high, size)):
            block = pl.ds(start, BLOCK)
            if count < BLOCK:
                chol[pl.ds(start + count, BLOCK - count)] = jnp.zeros(
                    (BLOCK - count, vectors, LANES), BF16
                )
            chol[pl.ds(start, count), :, 0:FULL] = raw_chol[pl.ds(start, count), :, 0:FULL]
            chol[block, :, FULL:LANES] = jnp.zeros((BLOCK, vectors, LANES - FULL), BF16)
            chol[pl.ds(start, count), :, FULL:NVIR] = raw_chol[pl.ds(start, count), :, FULL:NVIR]
            tiles.append(chol[block, :, FULL:LANES].reshape(BLOCK * vectors, LANES - FULL))
        made = jnp.dot(
            jnp.concatenate(tiles, axis=1), pack[...], preferred_element_type=F32
        )
        chol[pl.ds(low, BLOCK), :, FULL:LANES] = (
            made[:, 0:128].astype(BF16).reshape(BLOCK, vectors, LANES - FULL)
        )
        chol[pl.ds(high, BLOCK), :, FULL:LANES] = jnp.zeros((BLOCK, vectors, LANES - FULL), BF16)
        within = lax.rem(lax.broadcasted_iota(jnp.int32, (vectors, 128), 1), PART)
        for third in range(LAST[1]):
            found = [
                (row, first)
                for base, first in ((low, 128), (high, 256))
                for row in range(BLOCK)
                if base + row < NOCC and (base + row) // PART == third
            ]
            if found:
                kept = leftover[third]
                for row, first in found:
                    index = (row + (low if first == 128 else high)) % PART
                    part = made[row * vectors : (row + 1) * vectors, first : first + 128]
                    kept = jnp.where(within == index, part, kept)
                leftover[third] = kept

    def place_leftover():
        lanes = lax.broadcasted_iota(jnp.int32, (vectors, 128), 1)
        for third in range(LAST[1]):
            for column in range(LAST[0]):
                row = SPARE + LAST[1] * column + third
                value = leftover[third]
                if column:
                    value = pltpu.roll(value, PART, 1)
                old = chol[row, :, FULL:LANES].astype(F32)
                chol[row, :, FULL:LANES] = jnp.where(lanes < PART, old, value).astype(BF16)

    def add_block(slots, block):
        rows = pl.ds(pl.multiple_of(block * BLOCK, BLOCK), BLOCK)
        left = chol[rows].reshape(BLOCK * vectors, LANES)
        right = jnp.concatenate(
            [greens[slot, walker, rows, :] for slot in slots for walker in range(2)], axis=0
        )
        total[...] += transposed_dot(left, right)

    def forward(step, part, up, down):
        ring_copy(True, step, part).wait_recv()
        if up:
            ring_copy(True, step + 1, part).start()
        ring_copy(False, step, part).wait_recv()
        if down:
            ring_copy(False, step + 1, part).start()

    def upper_core():
        greet((1, -1), 0)
        for block in range(BLOCKS // 2):
            chol_copy(block).start()
            chol_copy(block + BLOCKS // 2).start()
        own_walker(1)
        pl.semaphore_wait(barrier, 3)
        rows_to_lower().start()
        for part in LAST_UP + LAST_DOWN:
            if part in LAST_DOWN:
                block_to_upper(part).wait_recv()
            ring_copy(True, 1, part).start()
            ring_copy(False, 1, part).start()

        total[...] = jnp.zeros_like(total)
        leftover[...] = jnp.zeros_like(leftover)
        packing()

        @pl.loop(1, chips)
        def _(slot):
            for walker in range(2):
                greens[slot, walker, SENT:ROWS, 0:FULL] = jnp.zeros((ROWS - SENT, FULL), BF16)
                greens[slot, walker, ROWS // 2 : ROWS, FULL:LANES] = jnp.zeros(
                    (ROWS // 2, LANES - FULL), BF16
                )

        greens[0, 0, SENT:ROWS, 0:FULL] = jnp.zeros((ROWS - SENT, FULL), BF16)
        greens[0, 0, ROWS // 2 : ROWS, FULL:LANES] = jnp.zeros((ROWS // 2, LANES - FULL), BF16)

        for step in (1, 2):
            for part in range(len(CHUNKS)):
                forward(step, part, True, True)
                if (step, part) in CLEANED:
                    clean_pair(CLEANED[step, part])
        place_leftover()

        @pl.loop(3, half - 1)
        def _(step):
            pair = lax.div(step - 1, 2)
            second = lax.rem(step - 1, 2)
            slots = (2 * pair - 1, 2 * pair, half + 2 * pair - 1, half + 2 * pair)
            for part in range(len(CHUNKS)):
                forward(step, part, True, True)
                for block in HALF_BLOCKS[part]:
                    add_block(slots, second * (BLOCKS // 2) + block)

            @pl.when(second == 1)
            def _():
                places = (slots[0], slots[1], chips + 1 - 2 * pair, chips - 2 * pair)
                keep_rows(places)
                for place in places:
                    back_copy(place).start()

        step = half - 1
        slots = (half - 3, half - 2, 2 * half - 3, 2 * half - 2)
        for part in range(len(CHUNKS)):
            forward(step, part, part in LAST_UP, part in LAST_DOWN)
            for block in ALL_BLOCKS[part]:
                add_block(slots, block)
        places = (half - 3, half - 2, half + 3, half + 2)
        keep_rows(places)
        for place in places:
            back_copy(place).start()

        slots = (half, half - 1, 2 * half - 1, 0)
        for part in range(len(CHUNKS)):
            ring_copy(part in LAST_UP, half, part).wait_recv()
            for block in LAST_BLOCKS[part]:
                add_block(slots, block)
        keep_rows((half, half - 1, half + 1, 0))
        for place in (half, half - 1, half + 1):
            back_copy(place).start()
        inbox[lax.rem(me, 2), lax.div(me, 2)] = message[0]

        rows_to_lower().wait_send()
        for part in range(len(CHUNKS)):
            ring_copy(True, 1, part).wait_send()
            ring_copy(False, 1, part).wait_send()

        @pl.loop(2, half)
        def _(step):
            for part in range(len(CHUNKS)):
                ring_copy(True, step, part).wait_send()
                ring_copy(False, step, part).wait_send()

        for part in range(len(CHUNKS)):
            ring_copy(part in LAST_UP, half, part).wait_send()
        corr_to_upper().wait_recv()
        inbox_swap(0).wait_recv()
        for offset in range(1, chips):
            back_copy(offset).wait_send()
        for offset in range(1, chips):
            back_wait(offset)
        inbox_swap(0).start()
        write_bias(corr_in[1:2, 0:1], inbox[...], peer_inbox[...], True)
        inbox_swap(0).wait_send()

    up_hops = members // 2
    down_hops = members - 1 - up_hops

    def hop_copy(buffer, send, recv, up, number):
        source = (number - 1) if up else (members - (number - 1)) % members
        target = number if up else members - number
        return pltpu.make_async_remote_copy(
            src_ref=buffer.at[0, source],
            dst_ref=buffer.at[0, target],
            send_sem=send.at[target],
            recv_sem=recv.at[target],
            device_id=chip(STRIDE if up else -STRIDE),
            device_id_type=MESH,
        )

    both_ways = (2, members // 2)

    def shift_of(place, member):
        return -SHIFTS[place] if place == 2 and member >= members // 2 else SHIFTS[place]

    def member_of(place, member):
        return 0 if (place, member) == both_ways else member

    def near_copy(buffer, send, recv, place, member):
        return pltpu.make_async_remote_copy(
            src_ref=buffer.at[0, member_of(place, member)],
            dst_ref=buffer.at[place, member],
            send_sem=send.at[place, member],
            recv_sem=recv.at[place, member],
            device_id=chip(shift_of(place, member)),
            device_id_type=MESH,
        )

    def start_spread(buffer, sems):
        send, recv, send_near, recv_near = sems
        hop_copy(buffer, send, recv, True, 1).start()
        if down_hops:
            hop_copy(buffer, send, recv, False, 1).start()
        for place in (1, 2, 3):
            near_copy(buffer, send_near, recv_near, place, 0).start()
        near_copy(buffer, send_near, recv_near, *both_ways).start()

    def hop_members(number):
        found = [number] if number <= up_hops else []
        return found + ([members - number] if number <= down_hops else [])

    def take_hop(buffer, sems, number):
        send, recv, send_near, recv_near = sems
        if number <= up_hops:
            hop_copy(buffer, send, recv, True, number).wait_recv()
            if number < up_hops:
                hop_copy(buffer, send, recv, True, number + 1).start()
        if number <= down_hops:
            hop_copy(buffer, send, recv, False, number).wait_recv()
            if number < down_hops:
                hop_copy(buffer, send, recv, False, number + 1).start()
        for member in hop_members(number):
            for place in (2, 1, 3):
                if (place, member) != both_ways:
                    near_copy(buffer, send_near, recv_near, place, member).start()

    def take_near(buffer, sems, member):
        for place in (1, 2, 3):
            near_copy(buffer, sems[2], sems[3], place, member).wait_recv()

    def end_spread(buffer, sems):
        send, recv, send_near, recv_near = sems
        for number in range(1, up_hops + 1):
            hop_copy(buffer, send, recv, True, number).wait_send()
        for number in range(1, down_hops + 1):
            hop_copy(buffer, send, recv, False, number).wait_send()
        for member in range(members):
            for place in (1, 2, 3):
                near_copy(buffer, send_near, recv_near, place, member).wait_send()

    def add_determinants(member):
        table = jnp.concatenate([tables[place, member] for place in range(4)], axis=1).astype(F32)
        width = table.shape[1]
        amplitude = table[8:9] + table[9:10] + table[10:11]
        orbital = lax.broadcasted_iota(jnp.int32, (NAO, width), 0).astype(F32)
        particle_hot = jnp.concatenate(
            [
                jnp.where(orbital == table[4 + row : 5 + row], 1.0, 0.0).astype(BF16)
                for row in range(MAXEXC)
            ],
            axis=1,
        )
        picked = jnp.dot(active[:, 0:NAV], particle_hot, preferred_element_type=F32)
        masks = [orbital == table[column : column + 1] for column in range(MAXEXC)]
        pieces = []
        for walker in range(2):
            rows = slice(walker * NAO, (walker + 1) * NAO)
            matrix = []
            for row in range(MAXEXC):
                own = picked[rows, row * width : (row + 1) * width]
                entries = [
                    jnp.sum(jnp.where(masks[column], own, 0.0), axis=0, keepdims=True)
                    for column in range(MAXEXC)
                ]
                entries[row] = jnp.where(table[4 + row : 5 + row] < 0.0, 1.0, entries[row])
                matrix.append(entries)
            ratios, pullback = jax.vjp(minor_determinant, matrix)
            cofactors = pullback(jnp.ones_like(ratios))[0]
            corr_total[walker] += ratios * amplitude
            uppers, lowers = [], []
            for row in range(MAXEXC):
                spread = jnp.zeros((NAO, width), F32)
                for column in range(MAXEXC):
                    spread = jnp.where(masks[column], cofactors[row][column] * amplitude, spread)
                upper = spread.astype(BF16)
                uppers.append(upper)
                lowers.append((spread - upper.astype(F32)).astype(BF16))
            pieces += [jnp.concatenate(uppers, axis=1), jnp.concatenate(lowers, axis=1)]
        grad_total[:, 0:NAV] += transposed_dot(jnp.concatenate(pieces, axis=0), particle_hot)

    def finish_gradient():
        for walker in range(2):
            start = 2 * walker * NAO
            whole = grad_total[start : start + NAO, :] + grad_total[start + NAO : start + 2 * NAO, :]
            packed = whole[0 : NAO // 2] + pltpu.roll(whole[NAO // 2 : NAO], NAV, 1)
            gradients[0, 0, walker] = packed.astype(BF16)

    def add_active(member):
        lanes = lax.broadcasted_iota(jnp.int32, (NAO // 2, 128), 1)
        unpacked = []
        for place in range(4):
            for walker in range(2):
                packed = gradients[place, member, walker].astype(F32)
                unpacked.append(
                    (
                        jnp.where(lanes < NAV, packed, 0.0).astype(BF16),
                        jnp.where(lanes < NAV, pltpu.roll(packed, NAV, 1), 0.0).astype(BF16),
                    )
                )
        for block in range(NAO // BLOCK):
            left = active_chol[pl.ds(block * BLOCK, BLOCK)].reshape(BLOCK * vectors, 128)
            side, inner = divmod(block * BLOCK, NAO // 2)
            right = jnp.concatenate(
                [halves[side][inner : inner + BLOCK] for halves in unpacked], axis=0
            )
            total[...] += transposed_dot(left, right)
        places = [(shift_of(place, member) + STRIDE * member_of(place, member)) % chips for place in range(4)]
        keep_rows(places)
        for place in places:
            if place:
                back_copy(place).start()

    table_sems = (table_send, table_recv, table_send_near, table_recv_near)
    grad_sems = (grad_send, grad_recv, grad_send_near, grad_recv_near)

    def lower_core():
        chol_part = pltpu.make_async_copy(
            chol_ref.at[pl.ds(NOCC - NAO, NAO), :, pl.ds(0, 128)], active_chol, chol_sem.at[0]
        )
        chol_part.start()
        partners = (1, -1, 2, -2, STRIDE, -STRIDE)
        greet(partners, 1)
        own_walker(0)
        order = order_ref[...]
        live = lax.broadcasted_iota(jnp.int32, (MAXEXC, order.shape[1]), 0) < order
        table_build[...] = jnp.zeros_like(table_build)
        table_build[0:4, :] = jnp.where(live, hole_ref[...], -1).astype(F32)
        table_build[4:8, :] = jnp.where(live, particle_ref[...], -1).astype(F32)
        amp = amp_ref[...]
        high = amp.astype(BF16).astype(F32)
        middle = (amp - high).astype(BF16).astype(F32)
        table_build[8:9, :] = high
        table_build[9:10, :] = middle
        table_build[10:11, :] = amp - high - middle
        tables[0, 0] = table_build[...].astype(BF16)

        pl.semaphore_wait(barrier, len(partners) + 1)
        for part in LAST_DOWN:
            block_to_upper(part).start()
        start_spread(tables, table_sems)

        total[...] = jnp.zeros_like(total)
        grad_total[...] = jnp.zeros_like(grad_total)
        corr_total[...] = jnp.zeros_like(corr_total)
        shift_rows = lax.broadcasted_iota(jnp.int32, (NAO, ROWS // 2), 0)
        shift_columns = lax.broadcasted_iota(jnp.int32, (NAO, ROWS // 2), 1)
        offset = NOCC - NAO - ROWS // 2
        shift = (shift_columns == shift_rows + offset).astype(F32).astype(BF16)
        active[0:NAO, :] = jnp.dot(
            shift, greens[0, 0, ROWS // 2 : ROWS, 0:128], preferred_element_type=F32
        ).astype(BF16)
        rows_to_lower().wait_recv()
        active[NAO : 2 * NAO, :] = jnp.dot(
            shift, peer_rows[...], preferred_element_type=F32
        ).astype(BF16)

        late = [0]
        for number in range(1, up_hops + 1):
            take_hop(tables, table_sems, number)
            for member in late:
                take_near(tables, table_sems, member)
                add_determinants(member)
            late = hop_members(number)
        for member in late:
            take_near(tables, table_sems, member)
            add_determinants(member)
        finish_gradient()
        start_spread(gradients, grad_sems)

        for walker in range(2):
            corr_out[walker : walker + 1, :] = jnp.broadcast_to(
                1.0 + jnp.sum(corr_total[walker], axis=1, keepdims=True), (1, 128)
            )
        chol_part.wait()

        late = [0]
        for number in range(1, up_hops + 1):
            take_hop(gradients, grad_sems, number)
            if number == 1:
                corr_to_upper().start()
            for member in late:
                take_near(gradients, grad_sems, member)
                add_active(member)
            late = hop_members(number)
        for member in late:
            take_near(gradients, grad_sems, member)
            add_active(member)
        inbox[lax.rem(me, 2), lax.div(me, 2)] = message[0]

        end_spread(tables, table_sems)
        end_spread(gradients, grad_sems)
        for part in LAST_DOWN:
            block_to_upper(part).wait_send()
        corr_to_upper().wait_send()
        for offset in range(1, chips):
            back_copy(offset).wait_send()
        for offset in range(1, chips):
            back_wait(offset)
        inbox_swap(1).start()
        inbox_swap(1).wait()
        write_bias(corr_out[0:1, 0:1], peer_inbox[...], inbox[...], False)

    @pl.when(core == 1)
    def _():
        upper_core()

    @pl.when(core == 0)
    def _():
        lower_core()


def shards(greens, chol_vectors, hole_orbitals, particle_orbitals, excitation_order, amplitudes):
    chips = lax.axis_size("det")
    vectors = chol_vectors.shape[0]
    dets = hole_orbitals.shape[0]
    members = chips // STRIDE
    half = chips // 2
    dma = pltpu.SemaphoreType.DMA
    vmem = pl.BlockSpec(memory_space=pltpu.VMEM)
    corr, bias = pl.pallas_call(
        functools.partial(kernel, chips),
        out_shape=(
            jax.ShapeDtypeStruct((1, 128), F32),
            jax.ShapeDtypeStruct((chips * vectors // 128, 128), F32),
        ),
        in_specs=[vmem, pl.BlockSpec(memory_space=pl.ANY), vmem, vmem, vmem, vmem],
        out_specs=(vmem, vmem),
        scratch_shapes=[
            pltpu.VMEM((NOCC, vectors, NVIR), BF16),
            pltpu.VMEM((ROWS, vectors, LANES), BF16),
            pltpu.VMEM((NAO, vectors, 128), BF16),
            pltpu.VMEM((chips, 2, ROWS, LANES), BF16),
            pltpu.VMEM((BLOCK * vectors, BATCH * BLOCK), F32),
            pltpu.VMEM((4, members, 16, dets), BF16),
            pltpu.VMEM((4, members, 2, NAO // 2, 128), BF16),
            pltpu.VMEM((16, dets), F32),
            pltpu.VMEM((ROWS // 2, 128), BF16),
            pltpu.VMEM((2 * NAO, 128), BF16),
            pltpu.VMEM((4 * NAO, 128), F32),
            pltpu.VMEM((2, 1, 4 * dets), F32),
            pltpu.VMEM((chips, 1, 128), F32),
            pltpu.VMEM((2, half, 1, 128), F32),
            pltpu.VMEM((2, half, 1, 128), F32),
            pltpu.VMEM((8, 128), F32),
            pltpu.VMEM((8, 128), F32),
            pltpu.VMEM((256, 384), BF16),
            pltpu.VMEM((LAST[1], vectors, 128), F32),
            dma((BLOCKS,)),
            dma((4 + len(CHUNKS) // 2,)),
            dma((4 + len(CHUNKS) // 2,)),
            dma((2, half + 1, len(CHUNKS))),
            dma((2, half + 1, len(CHUNKS))),
            dma((members,)),
            dma((members,)),
            dma((4, members)),
            dma((4, members)),
            dma((members,)),
            dma((members,)),
            dma((4, members)),
            dma((4, members)),
            dma((chips,)),
            dma((chips,)),
        ],
        compiler_params=pltpu.CompilerParams(
            collective_id=0, has_side_effects=True, vmem_limit_bytes=56 * 1024 * 1024
        ),
        name="walker_ring",
    )(
        jnp.transpose(greens, (0, 2, 1)).reshape(NOCC, NVIR),
        jnp.transpose(chol_vectors, (2, 0, 1)),
        jnp.transpose(hole_orbitals),
        jnp.transpose(particle_orbitals),
        excitation_order.reshape(1, dets),
        amplitudes.reshape(1, dets),
    )
    return (corr[0, 0:1], bias.reshape(1, chips * vectors))


def solution(mesh):
    placed = (
        P(("grp", "det", "wlk"), None, None),
        P(("grp", "det"), None, None),
        P(("grp", "det"), None),
        P(("grp", "det"), None),
        P(("grp", "det")),
        P(("grp", "det")),
    )
    return jax.shard_map(
        shards,
        mesh=mesh,
        in_specs=placed,
        out_specs=(P(("grp", "det", "wlk")), P(("grp", "det", "wlk"), None)),
        check_vma=False,
    )
```

```python
import functools

import jax
import jax.numpy as jnp
from jax import lax
from jax.experimental import pallas as pl
from jax.experimental.pallas import tpu as pltpu
from jax.sharding import PartitionSpec as P

NOCC = 150
NVIR = 450
NAO = 64
NAV = 64
MAXEXC = 4

MESH = pl.DeviceIdType.MESH
F32 = jnp.float32
BF16 = jnp.bfloat16

ROWS = 160
SENT = 152
LANES = 512
BLOCK = 16
BLOCKS = ROWS // BLOCK
BATCH = 8
FULL = NVIR // 128 * 128
PART = 64
SPARE = NOCC - ROWS // 2
LAST = (NVIR - FULL - PART, -(-NOCC // PART))
CHUNKS = (
    (1, 80, 72, 384),
    (0, 80, 72, 384),
    (1, 0, 48, 512),
    (0, 0, 48, 512),
    (1, 48, 32, 512),
    (0, 48, 32, 512),
)
LAST_UP = (0, 2, 4)
LAST_DOWN = (1, 3, 5)
CLEANED = {(1, 1): 0, (1, 2): 1, (1, 4): 2, (2, 0): 3, (2, 2): 4}
HALF_BLOCKS = ((0,), (1,), (2,), (3,), (4,), ())
ALL_BLOCKS = ((0, 1), (2,), (3, 4), (5,), (6, 7), (8, 9))
LAST_BLOCKS = ((), (5, 6, 7, 8, 9), (), (0, 1, 2), (), (3, 4))
STRIDE = 4
SHIFTS = (0, 1, 2, -1)


def minor_determinant(matrix):
    column_pairs = ((0, 1), (0, 2), (0, 3), (1, 2), (1, 3), (2, 3))
    parity = (1.0, -1.0, 1.0, 1.0, -1.0, 1.0)
    result = 0.0
    for number in range(6):
        first_column, second_column = column_pairs[number]
        third_column, fourth_column = column_pairs[5 - number]
        uppers = (
            matrix[0][first_column] * matrix[1][second_column]
            - matrix[1][first_column] * matrix[0][second_column]
        )
        lowers = (
            matrix[2][third_column] * matrix[3][fourth_column]
            - matrix[3][third_column] * matrix[2][fourth_column]
        )
        result = result + parity[number] * uppers * lowers
    return result


def transposed_dot(left, right):
    return lax.dot_general(left, right, (((1,), (1,)), ((), ())), preferred_element_type=F32)


def kernel(
    chips,
    green_ref,
    chol_ref,
    hole_ref,
    particle_ref,
    order_ref,
    amp_ref,
    corr_ref,
    bias_ref,
    raw_chol,
    chol,
    active_chol,
    greens,
    total,
    tables,
    gradients,
    table_build,
    peer_rows,
    active,
    grad_total,
    corr_total,
    message,
    inbox,
    peer_inbox,
    corr_out,
    corr_in,
    pack,
    leftover,
    chol_sem,
    swap_send,
    swap_recv,
    ring_send,
    ring_recv,
    table_send,
    table_recv,
    table_send_near,
    table_recv_near,
    grad_send,
    grad_recv,
    grad_send_near,
    grad_recv_near,
    back_send,
    back_recv,
    near_sem,
    far_sem,
):
    half = chips // 2
    members = chips // STRIDE
    vectors = chol.shape[1]
    me = lax.axis_index("det")
    core = lax.axis_index("wlk")
    barrier = pltpu.get_barrier_semaphore()

    def chip(offset):
        return {"det": lax.rem(me + offset + chips, chips)}

    def greet(offsets, other):
        for offset in offsets:
            pl.semaphore_signal(barrier, inc=1, device_id=chip(offset), device_id_type=MESH)
        pl.semaphore_signal(barrier, inc=1, device_id={"wlk": other}, device_id_type=MESH)

    def swap_copy(source, target, number, other):
        return pltpu.make_async_remote_copy(
            src_ref=source,
            dst_ref=target,
            send_sem=swap_send.at[number],
            recv_sem=swap_recv.at[number],
            device_id={"wlk": other},
            device_id_type=MESH,
        )

    def block_to_upper(part):
        _, start, size, lanes = CHUNKS[part]
        block = greens.at[0, 0, pl.ds(start, size), pl.ds(0, lanes)]
        return swap_copy(block, block, 4 + part // 2, 1)

    def rows_to_lower():
        rows = greens.at[0, 1, pl.ds(ROWS // 2, ROWS // 2), pl.ds(0, 128)]
        return swap_copy(rows, peer_rows, 1, 0)

    def inbox_swap(other):
        return swap_copy(inbox, peer_inbox, 2, other)

    def corr_to_upper():
        return swap_copy(corr_out, corr_in, 3, 1)

    def back_copy(offset):
        return pltpu.make_async_remote_copy(
            src_ref=message.at[offset],
            dst_ref=inbox.at[lax.rem(me, 2), lax.div(me, 2)],
            send_sem=back_send.at[offset],
            recv_sem=back_recv.at[offset],
            device_id={"det": lax.rem(me - offset + chips, chips)},
            device_id_type=MESH,
        )

    def back_wait(offset):
        sender = lax.rem(me + offset, chips)
        pltpu.make_async_remote_copy(
            src_ref=message.at[offset],
            dst_ref=inbox.at[lax.rem(sender, 2), lax.div(sender, 2)],
            send_sem=back_send.at[offset],
            recv_sem=back_recv.at[offset],
            device_id=chip(offset),
            device_id_type=MESH,
        ).wait_recv()

    def take_total():
        columns = lax.broadcasted_iota(jnp.int32, (vectors, BATCH * BLOCK), 1)
        kept = jnp.zeros((vectors, BATCH * BLOCK), F32)
        for row in range(BLOCK):
            part = total[pl.ds(row * vectors, vectors), :]
            kept = kept + jnp.where(lax.rem(columns, BLOCK) == row, part, 0.0)
        total[...] = jnp.zeros_like(total)
        turned = kept.T
        return [
            jnp.sum(turned[number * BLOCK : (number + 1) * BLOCK, :], axis=0, keepdims=True)
            for number in range(BATCH)
        ]

    def keep_rows(places):
        rows = take_total()
        for number, place in enumerate(places):
            message[place] = jnp.concatenate([rows[2 * number], rows[2 * number + 1]], axis=1)

    def own_walker(index):
        greens[0, index] = jnp.zeros((ROWS, LANES), BF16)
        greens[0, index, 0:NOCC, 0:NVIR] = green_ref[...]
        tile = greens[0, index, :, FULL:LANES].astype(F32)
        middle = ROWS // 2
        lanes = lax.broadcasted_iota(jnp.int32, tile.shape, 1)
        rows = lax.broadcasted_iota(jnp.int32, tile.shape, 0)
        further = pltpu.roll(tile[middle:], PART, 1)
        packed = jnp.where(lanes[:middle] < PART, tile[:middle], further)
        for column in range(LAST[0]):
            for third in range(LAST[1]):
                match = (lanes == rows + (1 - third) * PART) & (lanes >= PART)
                row = jnp.sum(
                    jnp.where(match, tile[:, PART + column : PART + column + 1], 0.0),
                    axis=0,
                    keepdims=True,
                )
                place = SPARE + LAST[1] * column + third
                packed = jnp.where(
                    (rows[:middle] == place) & (lanes[:middle] >= PART), row, packed
                )
        greens[0, index, 0:middle, FULL:LANES] = packed.astype(BF16)
        greens[0, index, middle:ROWS, FULL:LANES] = jnp.zeros((middle, LANES - FULL), BF16)

    def write_bias(corr, whole, term, upper):
        even = corr * whole[0].reshape(half, 128) + term[0].reshape(half, 128)
        odd = corr * whole[1].reshape(half, 128) + term[1].reshape(half, 128)
        lanes = lax.broadcasted_iota(jnp.int32, even.shape, 1)
        if upper:
            even = pltpu.roll(even, vectors, 1)
        else:
            odd = pltpu.roll(odd, vectors, 1)
        bias_ref[...] = jnp.where(lanes < vectors, even, odd)
        corr_ref[...] = jnp.broadcast_to(corr, corr_ref.shape)

    def ring_copy(up, step, part):
        walker, start, size, lanes = CHUNKS[part]
        if up:
            source, target = step - 1, step
        elif isinstance(step, int):
            source = half + step - 1 if step > 1 else 0
            target = half + step if step < half else half
        else:
            source, target = half + step - 1, half + step
        return pltpu.make_async_remote_copy(
            src_ref=greens.at[source, walker, pl.ds(start, size), pl.ds(0, lanes)],
            dst_ref=greens.at[target, walker, pl.ds(start, size), pl.ds(0, lanes)],
            send_sem=ring_send.at[0 if up else 1, step, part],
            recv_sem=ring_recv.at[0 if up else 1, step, part],
            device_id=chip(1 if up else -1),
            device_id_type=MESH,
        )

    def chol_copy(block):
        start = block * BLOCK
        size = min(BLOCK, NOCC - start)
        return pltpu.make_async_copy(
            chol_ref.at[pl.ds(start, size)], raw_chol.at[pl.ds(start, size)], chol_sem.at[block]
        )

    def packing():
        rows = lax.broadcasted_iota(jnp.int32, pack.shape, 0)
        columns = lax.broadcasted_iota(jnp.int32, pack.shape, 1)
        within = lax.rem(columns, 128)
        last = PART + jnp.where(within < PART, 1, 0)
        source = jnp.where(
            columns < 128,
            jnp.where(columns < PART, columns, columns + 128 - PART),
            jnp.where(columns < 256, last, last + 128),
        )
        pack[...] = jnp.where(rows == source, 1.0, 0.0).astype(BF16)

    def clean_pair(pair):
        low = pair * BLOCK
        high = ROWS // 2 + low
        size = min(BLOCK, NOCC - high)
        chol_copy(pair).wait()
        chol_copy(pair + BLOCKS // 2).wait()
        tiles = []
        for start, count in ((low, BLOCK), (high, size)):
            block = pl.ds(start, BLOCK)
            if count < BLOCK:
                chol[pl.ds(start + count, BLOCK - count)] = jnp.zeros(
                    (BLOCK - count, vectors, LANES), BF16
                )
            chol[pl.ds(start, count), :, 0:FULL] = raw_chol[pl.ds(start, count), :, 0:FULL]
            chol[block, :, FULL:LANES] = jnp.zeros((BLOCK, vectors, LANES - FULL), BF16)
            chol[pl.ds(start, count), :, FULL:NVIR] = raw_chol[pl.ds(start, count), :, FULL:NVIR]
            tiles.append(chol[block, :, FULL:LANES].reshape(BLOCK * vectors, LANES - FULL))
        made = jnp.dot(
            jnp.concatenate(tiles, axis=1), pack[...], preferred_element_type=F32
        )
        chol[pl.ds(low, BLOCK), :, FULL:LANES] = (
            made[:, 0:128].astype(BF16).reshape(BLOCK, vectors, LANES - FULL)
        )
        chol[pl.ds(high, BLOCK), :, FULL:LANES] = jnp.zeros((BLOCK, vectors, LANES - FULL), BF16)
        within = lax.rem(lax.broadcasted_iota(jnp.int32, (vectors, 128), 1), PART)
        for third in range(LAST[1]):
            found = [
                (row, first)
                for base, first in ((low, 128), (high, 256))
                for row in range(BLOCK)
                if base + row < NOCC and (base + row) // PART == third
            ]
            if found:
                kept = leftover[third]
                for row, first in found:
                    index = (row + (low if first == 128 else high)) % PART
                    part = made[row * vectors : (row + 1) * vectors, first : first + 128]
                    kept = jnp.where(within == index, part, kept)
                leftover[third] = kept

    def place_leftover():
        lanes = lax.broadcasted_iota(jnp.int32, (vectors, 128), 1)
        for third in range(LAST[1]):
            for column in range(LAST[0]):
                row = SPARE + LAST[1] * column + third
                value = leftover[third]
                if column:
                    value = pltpu.roll(value, PART, 1)
                old = chol[row, :, FULL:LANES].astype(F32)
                chol[row, :, FULL:LANES] = jnp.where(lanes < PART, old, value).astype(BF16)

    def add_block(slots, block):
        rows = pl.ds(pl.multiple_of(block * BLOCK, BLOCK), BLOCK)
        left = chol[rows].reshape(BLOCK * vectors, LANES)
        right = jnp.concatenate(
            [greens[slot, walker, rows, :] for slot in slots for walker in range(2)], axis=0
        )
        total[...] += transposed_dot(left, right)

    def forward(step, part, up, down):
        ring_copy(True, step, part).wait_recv()
        if up:
            ring_copy(True, step + 1, part).start()
        ring_copy(False, step, part).wait_recv()
        if down:
            ring_copy(False, step + 1, part).start()

    def upper_core():
        greet((1, -1), 0)
        for block in range(BLOCKS // 2):
            chol_copy(block).start()
            chol_copy(block + BLOCKS // 2).start()
        own_walker(1)
        pl.semaphore_wait(barrier, 3)
        rows_to_lower().start()
        for part in LAST_UP + LAST_DOWN:
            if part in LAST_DOWN:
                block_to_upper(part).wait_recv()
            ring_copy(True, 1, part).start()
            ring_copy(False, 1, part).start()

        total[...] = jnp.zeros_like(total)
        leftover[...] = jnp.zeros_like(leftover)
        packing()

        @pl.loop(1, chips)
        def _(slot):
            for walker in range(2):
                greens[slot, walker, SENT:ROWS, 0:FULL] = jnp.zeros((ROWS - SENT, FULL), BF16)
                greens[slot, walker, ROWS // 2 : ROWS, FULL:LANES] = jnp.zeros(
                    (ROWS // 2, LANES - FULL), BF16
                )

        greens[0, 0, SENT:ROWS, 0:FULL] = jnp.zeros((ROWS - SENT, FULL), BF16)
        greens[0, 0, ROWS // 2 : ROWS, FULL:LANES] = jnp.zeros((ROWS // 2, LANES - FULL), BF16)

        for step in (1, 2):
            for part in range(len(CHUNKS)):
                forward(step, part, True, True)
                if (step, part) in CLEANED:
                    clean_pair(CLEANED[step, part])
        place_leftover()

        @pl.loop(3, half - 1)
        def _(step):
            pair = lax.div(step - 1, 2)
            second = lax.rem(step - 1, 2)
            slots = (2 * pair - 1, 2 * pair, half + 2 * pair - 1, half + 2 * pair)
            for part in range(len(CHUNKS)):
                forward(step, part, True, True)
                for block in HALF_BLOCKS[part]:
                    add_block(slots, second * (BLOCKS // 2) + block)

            @pl.when(second == 1)
            def _():
                places = (slots[0], slots[1], chips + 1 - 2 * pair, chips - 2 * pair)
                keep_rows(places)
                for place in places:
                    back_copy(place).start()

        step = half - 1
        slots = (half - 3, half - 2, 2 * half - 3, 2 * half - 2)
        for part in range(len(CHUNKS)):
            forward(step, part, part in LAST_UP, part in LAST_DOWN)
            for block in ALL_BLOCKS[part]:
                add_block(slots, block)
        places = (half - 3, half - 2, half + 3, half + 2)
        keep_rows(places)
        for place in places:
            back_copy(place).start()

        slots = (half, half - 1, 2 * half - 1, 0)
        for part in range(len(CHUNKS)):
            ring_copy(part in LAST_UP, half, part).wait_recv()
            for block in LAST_BLOCKS[part]:
                add_block(slots, block)
        keep_rows((half, half - 1, half + 1, 0))
        for place in (half, half - 1, half + 1):
            back_copy(place).start()
        inbox[lax.rem(me, 2), lax.div(me, 2)] = message[0]

        rows_to_lower().wait_send()
        for part in range(len(CHUNKS)):
            ring_copy(True, 1, part).wait_send()
            ring_copy(False, 1, part).wait_send()

        @pl.loop(2, half)
        def _(step):
            for part in range(len(CHUNKS)):
                ring_copy(True, step, part).wait_send()
                ring_copy(False, step, part).wait_send()

        for part in range(len(CHUNKS)):
            ring_copy(part in LAST_UP, half, part).wait_send()
        corr_to_upper().wait_recv()
        inbox_swap(0).wait_recv()
        for offset in range(1, chips):
            back_copy(offset).wait_send()
        for offset in range(1, chips):
            back_wait(offset)
        inbox_swap(0).start()
        write_bias(corr_in[1:2, 0:1], inbox[...], peer_inbox[...], True)
        inbox_swap(0).wait_send()

    up_hops = members // 2
    down_hops = members - 1 - up_hops

    def hop_copy(buffer, send, recv, up, number):
        source = (number - 1) if up else (members - (number - 1)) % members
        target = number if up else members - number
        return pltpu.make_async_remote_copy(
            src_ref=buffer.at[0, source],
            dst_ref=buffer.at[0, target],
            send_sem=send.at[target],
            recv_sem=recv.at[target],
            device_id=chip(STRIDE if up else -STRIDE),
            device_id_type=MESH,
        )

    both_ways = (2, members // 2)

    def shift_of(place, member):
        return -SHIFTS[place] if place == 2 and member >= members // 2 else SHIFTS[place]

    def member_of(place, member):
        return 0 if (place, member) == both_ways else member

    def near_copy(buffer, send, recv, place, member):
        return pltpu.make_async_remote_copy(
            src_ref=buffer.at[0, member_of(place, member)],
            dst_ref=buffer.at[place, member],
            send_sem=send.at[place, member],
            recv_sem=recv.at[place, member],
            device_id=chip(shift_of(place, member)),
            device_id_type=MESH,
        )

    def start_spread(buffer, sems):
        send, recv, send_near, recv_near = sems
        hop_copy(buffer, send, recv, True, 1).start()
        if down_hops:
            hop_copy(buffer, send, recv, False, 1).start()
        for place in (1, 2, 3):
            near_copy(buffer, send_near, recv_near, place, 0).start()
        near_copy(buffer, send_near, recv_near, *both_ways).start()

    def hop_members(number):
        found = [number] if number <= up_hops else []
        return found + ([members - number] if number <= down_hops else [])

    def take_hop(buffer, sems, number):
        send, recv, send_near, recv_near = sems
        if number <= up_hops:
            hop_copy(buffer, send, recv, True, number).wait_recv()
            if number < up_hops:
                hop_copy(buffer, send, recv, True, number + 1).start()
        if number <= down_hops:
            hop_copy(buffer, send, recv, False, number).wait_recv()
            if number < down_hops:
                hop_copy(buffer, send, recv, False, number + 1).start()
        for member in hop_members(number):
            for place in (2, 1, 3):
                if (place, member) != both_ways:
                    near_copy(buffer, send_near, recv_near, place, member).start()

    def take_near(buffer, sems, member):
        for place in (1, 2, 3):
            near_copy(buffer, sems[2], sems[3], place, member).wait_recv()

    def end_spread(buffer, sems):
        send, recv, send_near, recv_near = sems
        for number in range(1, up_hops + 1):
            hop_copy(buffer, send, recv, True, number).wait_send()
        for number in range(1, down_hops + 1):
            hop_copy(buffer, send, recv, False, number).wait_send()
        for member in range(members):
            for place in (1, 2, 3):
                near_copy(buffer, send_near, recv_near, place, member).wait_send()

    def add_determinants(member):
        table = jnp.concatenate([tables[place, member] for place in range(4)], axis=1).astype(F32)
        width = table.shape[1]
        amplitude = table[8:9] + table[9:10] + table[10:11]
        orbital = lax.broadcasted_iota(jnp.int32, (NAO, width), 0).astype(F32)
        particle_hot = jnp.concatenate(
            [
                jnp.where(orbital == table[4 + row : 5 + row], 1.0, 0.0).astype(BF16)
                for row in range(MAXEXC)
            ],
            axis=1,
        )
        picked = jnp.dot(active[:, 0:NAV], particle_hot, preferred_element_type=F32)
        masks = [orbital == table[column : column + 1] for column in range(MAXEXC)]
        pieces = []
        for walker in range(2):
            rows = slice(walker * NAO, (walker + 1) * NAO)
            matrix = []
            for row in range(MAXEXC):
                own = picked[rows, row * width : (row + 1) * width]
                entries = [
                    jnp.sum(jnp.where(masks[column], own, 0.0), axis=0, keepdims=True)
                    for column in range(MAXEXC)
                ]
                entries[row] = jnp.where(table[4 + row : 5 + row] < 0.0, 1.0, entries[row])
                matrix.append(entries)
            ratios, pullback = jax.vjp(minor_determinant, matrix)
            cofactors = pullback(jnp.ones_like(ratios))[0]
            corr_total[walker] += ratios * amplitude
            uppers, lowers = [], []
            for row in range(MAXEXC):
                spread = jnp.zeros((NAO, width), F32)
                for column in range(MAXEXC):
                    spread = jnp.where(masks[column], cofactors[row][column] * amplitude, spread)
                upper = spread.astype(BF16)
                uppers.append(upper)
                lowers.append((spread - upper.astype(F32)).astype(BF16))
            pieces += [jnp.concatenate(uppers, axis=1), jnp.concatenate(lowers, axis=1)]
        grad_total[:, 0:NAV] += transposed_dot(jnp.concatenate(pieces, axis=0), particle_hot)

    def finish_gradient():
        for walker in range(2):
            start = 2 * walker * NAO
            whole = grad_total[start : start + NAO, :] + grad_total[start + NAO : start + 2 * NAO, :]
            packed = whole[0 : NAO // 2] + pltpu.roll(whole[NAO // 2 : NAO], NAV, 1)
            gradients[0, 0, walker] = packed.astype(BF16)

    def add_active(member):
        lanes = lax.broadcasted_iota(jnp.int32, (NAO // 2, 128), 1)
        unpacked = []
        for place in range(4):
            for walker in range(2):
                packed = gradients[place, member, walker].astype(F32)
                unpacked.append(
                    (
                        jnp.where(lanes < NAV, packed, 0.0).astype(BF16),
                        jnp.where(lanes < NAV, pltpu.roll(packed, NAV, 1), 0.0).astype(BF16),
                    )
                )
        for block in range(NAO // BLOCK):
            left = active_chol[pl.ds(block * BLOCK, BLOCK)].reshape(BLOCK * vectors, 128)
            side, inner = divmod(block * BLOCK, NAO // 2)
            right = jnp.concatenate(
                [halves[side][inner : inner + BLOCK] for halves in unpacked], axis=0
            )
            total[...] += transposed_dot(left, right)
        places = [(shift_of(place, member) + STRIDE * member_of(place, member)) % chips for place in range(4)]
        keep_rows(places)
        for place in places:
            if place:
                back_copy(place).start()

    table_sems = (table_send, table_recv, table_send_near, table_recv_near)
    grad_sems = (grad_send, grad_recv, grad_send_near, grad_recv_near)

    def lower_core():
        chol_part = pltpu.make_async_copy(
            chol_ref.at[pl.ds(NOCC - NAO, NAO), :, pl.ds(0, 128)], active_chol, chol_sem.at[0]
        )
        chol_part.start()
        greet((1, -1), 1)
        own_walker(0)
        pl.semaphore_wait(barrier, 3)
        for part in LAST_DOWN:
            block_to_upper(part).start()
        for offset in (1, -1):
            pl.semaphore_signal(near_sem, inc=1, device_id=chip(offset), device_id_type=MESH)

        order = order_ref[...]
        live = lax.broadcasted_iota(jnp.int32, (MAXEXC, order.shape[1]), 0) < order
        table_build[...] = jnp.zeros_like(table_build)
        table_build[0:4, :] = jnp.where(live, hole_ref[...], -1).astype(F32)
        table_build[4:8, :] = jnp.where(live, particle_ref[...], -1).astype(F32)
        amp = amp_ref[...]
        high = amp.astype(BF16).astype(F32)
        middle = (amp - high).astype(BF16).astype(F32)
        table_build[8:9, :] = high
        table_build[9:10, :] = middle
        table_build[10:11, :] = amp - high - middle
        tables[0, 0] = table_build[...].astype(BF16)

        pl.semaphore_wait(near_sem, 2)
        for offset in (2, -2):
            pl.semaphore_signal(far_sem, inc=1, device_id=chip(offset), device_id_type=MESH)
        pl.semaphore_wait(far_sem, 2)
        start_spread(tables, table_sems)

        total[...] = jnp.zeros_like(total)
        grad_total[...] = jnp.zeros_like(grad_total)
        corr_total[...] = jnp.zeros_like(corr_total)
        shift_rows = lax.broadcasted_iota(jnp.int32, (NAO, ROWS // 2), 0)
        shift_columns = lax.broadcasted_iota(jnp.int32, (NAO, ROWS // 2), 1)
        offset = NOCC - NAO - ROWS // 2
        shift = (shift_columns == shift_rows + offset).astype(F32).astype(BF16)
        active[0:NAO, :] = jnp.dot(
            shift, greens[0, 0, ROWS // 2 : ROWS, 0:128], preferred_element_type=F32
        ).astype(BF16)
        rows_to_lower().wait_recv()
        active[NAO : 2 * NAO, :] = jnp.dot(
            shift, peer_rows[...], preferred_element_type=F32
        ).astype(BF16)

        late = [0]
        for number in range(1, up_hops + 1):
            take_hop(tables, table_sems, number)
            for member in late:
                take_near(tables, table_sems, member)
                add_determinants(member)
            late = hop_members(number)
        for member in late:
            take_near(tables, table_sems, member)
            add_determinants(member)
        finish_gradient()
        start_spread(gradients, grad_sems)

        for walker in range(2):
            corr_out[walker : walker + 1, :] = jnp.broadcast_to(
                1.0 + jnp.sum(corr_total[walker], axis=1, keepdims=True), (1, 128)
            )
        chol_part.wait()

        late = [0]
        for number in range(1, up_hops + 1):
            take_hop(gradients, grad_sems, number)
            if number == 1:
                corr_to_upper().start()
            for member in late:
                take_near(gradients, grad_sems, member)
                add_active(member)
            late = hop_members(number)
        for member in late:
            take_near(gradients, grad_sems, member)
            add_active(member)
        inbox[lax.rem(me, 2), lax.div(me, 2)] = message[0]

        end_spread(tables, table_sems)
        end_spread(gradients, grad_sems)
        for part in LAST_DOWN:
            block_to_upper(part).wait_send()
        corr_to_upper().wait_send()
        for offset in range(1, chips):
            back_copy(offset).wait_send()
        for offset in range(1, chips):
            back_wait(offset)
        inbox_swap(1).start()
        inbox_swap(1).wait()
        write_bias(corr_out[0:1, 0:1], peer_inbox[...], inbox[...], False)

    @pl.when(core == 1)
    def _():
        upper_core()

    @pl.when(core == 0)
    def _():
        lower_core()


def shards(greens, chol_vectors, hole_orbitals, particle_orbitals, excitation_order, amplitudes):
    chips = lax.axis_size("det")
    vectors = chol_vectors.shape[0]
    dets = hole_orbitals.shape[0]
    members = chips // STRIDE
    half = chips // 2
    dma = pltpu.SemaphoreType.DMA
    vmem = pl.BlockSpec(memory_space=pltpu.VMEM)
    corr, bias = pl.pallas_call(
        functools.partial(kernel, chips),
        out_shape=(
            jax.ShapeDtypeStruct((1, 128), F32),
            jax.ShapeDtypeStruct((chips * vectors // 128, 128), F32),
        ),
        in_specs=[vmem, pl.BlockSpec(memory_space=pl.ANY), vmem, vmem, vmem, vmem],
        out_specs=(vmem, vmem),
        scratch_shapes=[
            pltpu.VMEM((NOCC, vectors, NVIR), BF16),
            pltpu.VMEM((ROWS, vectors, LANES), BF16),
            pltpu.VMEM((NAO, vectors, 128), BF16),
            pltpu.VMEM((chips, 2, ROWS, LANES), BF16),
            pltpu.VMEM((BLOCK * vectors, BATCH * BLOCK), F32),
            pltpu.VMEM((4, members, 16, dets), BF16),
            pltpu.VMEM((4, members, 2, NAO // 2, 128), BF16),
            pltpu.VMEM((16, dets), F32),
            pltpu.VMEM((ROWS // 2, 128), BF16),
            pltpu.VMEM((2 * NAO, 128), BF16),
            pltpu.VMEM((4 * NAO, 128), F32),
            pltpu.VMEM((2, 1, 4 * dets), F32),
            pltpu.VMEM((chips, 1, 128), F32),
            pltpu.VMEM((2, half, 1, 128), F32),
            pltpu.VMEM((2, half, 1, 128), F32),
            pltpu.VMEM((8, 128), F32),
            pltpu.VMEM((8, 128), F32),
            pltpu.VMEM((256, 384), BF16),
            pltpu.VMEM((LAST[1], vectors, 128), F32),
            dma((BLOCKS,)),
            dma((4 + len(CHUNKS) // 2,)),
            dma((4 + len(CHUNKS) // 2,)),
            dma((2, half + 1, len(CHUNKS))),
            dma((2, half + 1, len(CHUNKS))),
            dma((members,)),
            dma((members,)),
            dma((4, members)),
            dma((4, members)),
            dma((members,)),
            dma((members,)),
            dma((4, members)),
            dma((4, members)),
            dma((chips,)),
            dma((chips,)),
            pltpu.SemaphoreType.REGULAR,
            pltpu.SemaphoreType.REGULAR,
        ],
        compiler_params=pltpu.CompilerParams(
            collective_id=0, has_side_effects=True, vmem_limit_bytes=56 * 1024 * 1024
        ),
        name="walker_ring",
    )(
        jnp.transpose(greens, (0, 2, 1)).reshape(NOCC, NVIR),
        jnp.transpose(chol_vectors, (2, 0, 1)),
        jnp.transpose(hole_orbitals),
        jnp.transpose(particle_orbitals),
        excitation_order.reshape(1, dets),
        amplitudes.reshape(1, dets),
    )
    return (corr[0, 0:1], bias.reshape(1, chips * vectors))


def solution(mesh):
    placed = (
        P(("grp", "det", "wlk"), None, None),
        P(("grp", "det"), None, None),
        P(("grp", "det"), None),
        P(("grp", "det"), None),
        P(("grp", "det")),
        P(("grp", "det")),
    )
    return jax.shard_map(
        shards,
        mesh=mesh,
        in_specs=placed,
        out_specs=(P(("grp", "det", "wlk")), P(("grp", "det", "wlk"), None)),
        check_vma=False,
    )
```

```python
import functools

import jax
import jax.numpy as jnp
from jax import lax
from jax.experimental import pallas as pl
from jax.experimental.pallas import tpu as pltpu
from jax.sharding import PartitionSpec as P

NOCC = 150
NVIR = 450
NAO = 64
NAV = 64
MAXEXC = 4

MESH = pl.DeviceIdType.MESH
F32 = jnp.float32
BF16 = jnp.bfloat16

ROWS = 160
SENT = 152
LANES = 512
BLOCK = 16
BLOCKS = ROWS // BLOCK
BATCH = 8
FULL = NVIR // 128 * 128
PART = 64
SPARE = NOCC - ROWS // 2
LAST = (NVIR - FULL - PART, -(-NOCC // PART))
CHUNKS = (
    (1, 80, 72, 384),
    (0, 80, 72, 384),
    (1, 0, 48, 512),
    (0, 0, 48, 512),
    (1, 48, 32, 512),
    (0, 48, 32, 512),
)
LAST_UP = (0, 2, 4)
LAST_DOWN = (1, 3, 5)
CLEANED = {(1, 1): 0, (1, 2): 1, (1, 4): 2, (2, 0): 3, (2, 2): 4}
HALF_BLOCKS = ((0,), (1,), (2,), (3,), (4,), ())
ALL_BLOCKS = ((0, 1), (2,), (3, 4), (5,), (6, 7), (8, 9))
LAST_BLOCKS = ((), (5, 6, 7, 8, 9), (), (0, 1, 2), (), (3, 4))
STRIDE = 4
SHIFTS = (0, 1, 2, -1)


def minor_determinant(matrix):
    column_pairs = ((0, 1), (0, 2), (0, 3), (1, 2), (1, 3), (2, 3))
    parity = (1.0, -1.0, 1.0, 1.0, -1.0, 1.0)
    result = 0.0
    for number in range(6):
        first_column, second_column = column_pairs[number]
        third_column, fourth_column = column_pairs[5 - number]
        uppers = (
            matrix[0][first_column] * matrix[1][second_column]
            - matrix[1][first_column] * matrix[0][second_column]
        )
        lowers = (
            matrix[2][third_column] * matrix[3][fourth_column]
            - matrix[3][third_column] * matrix[2][fourth_column]
        )
        result = result + parity[number] * uppers * lowers
    return result


def transposed_dot(left, right):
    return lax.dot_general(left, right, (((1,), (1,)), ((), ())), preferred_element_type=F32)


def kernel(
    chips,
    green_ref,
    chol_ref,
    hole_ref,
    particle_ref,
    order_ref,
    amp_ref,
    corr_ref,
    bias_ref,
    raw_chol,
    chol,
    active_chol,
    greens,
    total,
    tables,
    gradients,
    table_build,
    peer_rows,
    active,
    grad_total,
    corr_total,
    message,
    inbox,
    peer_inbox,
    corr_out,
    corr_in,
    pack,
    leftover,
    chol_sem,
    swap_send,
    swap_recv,
    ring_send,
    ring_recv,
    table_send,
    table_recv,
    table_send_near,
    table_recv_near,
    grad_send,
    grad_recv,
    grad_send_near,
    grad_recv_near,
    back_send,
    back_recv,
    lower_send,
    lower_recv,
    near_sem,
    far_sem,
):
    half = chips // 2
    members = chips // STRIDE
    vectors = chol.shape[1]
    me = lax.axis_index("det")
    core = lax.axis_index("wlk")
    barrier = pltpu.get_barrier_semaphore()

    def chip(offset):
        return {"det": lax.rem(me + offset + chips, chips)}

    def greet(offsets, other):
        for offset in offsets:
            pl.semaphore_signal(barrier, inc=1, device_id=chip(offset), device_id_type=MESH)
        pl.semaphore_signal(barrier, inc=1, device_id={"wlk": other}, device_id_type=MESH)

    def swap_copy(source, target, number, other):
        return pltpu.make_async_remote_copy(
            src_ref=source,
            dst_ref=target,
            send_sem=swap_send.at[number],
            recv_sem=swap_recv.at[number],
            device_id={"wlk": other},
            device_id_type=MESH,
        )

    def block_to_upper(part):
        _, start, size, lanes = CHUNKS[part]
        block = greens.at[0, 0, pl.ds(start, size), pl.ds(0, lanes)]
        return swap_copy(block, block, 4 + part // 2, 1)

    def rows_to_lower():
        rows = greens.at[0, 1, pl.ds(ROWS // 2, ROWS // 2), pl.ds(0, 128)]
        return swap_copy(rows, peer_rows, 1, 0)

    def inbox_swap(other):
        return swap_copy(inbox, peer_inbox, 2, other)

    def corr_to_upper():
        return swap_copy(corr_out, corr_in, 3, 1)

    def back_copy(offset):
        return pltpu.make_async_remote_copy(
            src_ref=message.at[offset],
            dst_ref=inbox.at[lax.rem(me, 2), lax.div(me, 2)],
            send_sem=back_send.at[offset],
            recv_sem=back_recv.at[offset],
            device_id={"det": lax.rem(me - offset + chips, chips)},
            device_id_type=MESH,
        )

    def back_copy_lower(offset):
        return pltpu.make_async_remote_copy(
            src_ref=message.at[offset],
            dst_ref=peer_inbox.at[lax.rem(me, 2), lax.div(me, 2)],
            send_sem=lower_send.at[offset],
            recv_sem=lower_recv.at[offset],
            device_id={"det": lax.rem(me - offset + chips, chips), "wlk": 0},
            device_id_type=MESH,
        )

    def back_wait_lower(offset):
        sender = lax.rem(me + offset, chips)
        pltpu.make_async_remote_copy(
            src_ref=message.at[offset],
            dst_ref=peer_inbox.at[lax.rem(sender, 2), lax.div(sender, 2)],
            send_sem=lower_send.at[offset],
            recv_sem=lower_recv.at[offset],
            device_id={"det": sender, "wlk": 1},
            device_id_type=MESH,
        ).wait_recv()

    def back_wait(offset):
        sender = lax.rem(me + offset, chips)
        pltpu.make_async_remote_copy(
            src_ref=message.at[offset],
            dst_ref=inbox.at[lax.rem(sender, 2), lax.div(sender, 2)],
            send_sem=back_send.at[offset],
            recv_sem=back_recv.at[offset],
            device_id=chip(offset),
            device_id_type=MESH,
        ).wait_recv()

    def take_total():
        columns = lax.broadcasted_iota(jnp.int32, (vectors, BATCH * BLOCK), 1)
        kept = jnp.zeros((vectors, BATCH * BLOCK), F32)
        for row in range(BLOCK):
            part = total[pl.ds(row * vectors, vectors), :]
            kept = kept + jnp.where(lax.rem(columns, BLOCK) == row, part, 0.0)
        total[...] = jnp.zeros_like(total)
        turned = kept.T
        return [
            jnp.sum(turned[number * BLOCK : (number + 1) * BLOCK, :], axis=0, keepdims=True)
            for number in range(BATCH)
        ]

    def keep_rows(places):
        rows = take_total()
        for number, place in enumerate(places):
            message[place] = jnp.concatenate([rows[2 * number], rows[2 * number + 1]], axis=1)

    def own_walker(index):
        greens[0, index] = jnp.zeros((ROWS, LANES), BF16)
        greens[0, index, 0:NOCC, 0:NVIR] = green_ref[...]
        tile = greens[0, index, :, FULL:LANES].astype(F32)
        middle = ROWS // 2
        lanes = lax.broadcasted_iota(jnp.int32, tile.shape, 1)
        rows = lax.broadcasted_iota(jnp.int32, tile.shape, 0)
        further = pltpu.roll(tile[middle:], PART, 1)
        packed = jnp.where(lanes[:middle] < PART, tile[:middle], further)
        for column in range(LAST[0]):
            for third in range(LAST[1]):
                match = (lanes == rows + (1 - third) * PART) & (lanes >= PART)
                row = jnp.sum(
                    jnp.where(match, tile[:, PART + column : PART + column + 1], 0.0),
                    axis=0,
                    keepdims=True,
                )
                place = SPARE + LAST[1] * column + third
                packed = jnp.where(
                    (rows[:middle] == place) & (lanes[:middle] >= PART), row, packed
                )
        greens[0, index, 0:middle, FULL:LANES] = packed.astype(BF16)
        greens[0, index, middle:ROWS, FULL:LANES] = jnp.zeros((middle, LANES - FULL), BF16)

    def write_bias(corr, whole, term, upper):
        even = corr * whole[0].reshape(half, 128) + term[0].reshape(half, 128)
        odd = corr * whole[1].reshape(half, 128) + term[1].reshape(half, 128)
        lanes = lax.broadcasted_iota(jnp.int32, even.shape, 1)
        if upper:
            even = pltpu.roll(even, vectors, 1)
        else:
            odd = pltpu.roll(odd, vectors, 1)
        bias_ref[...] = jnp.where(lanes < vectors, even, odd)
        corr_ref[...] = jnp.broadcast_to(corr, corr_ref.shape)

    def ring_copy(up, step, part):
        walker, start, size, lanes = CHUNKS[part]
        if up:
            source, target = step - 1, step
        elif isinstance(step, int):
            source = half + step - 1 if step > 1 else 0
            target = half + step if step < half else half
        else:
            source, target = half + step - 1, half + step
        return pltpu.make_async_remote_copy(
            src_ref=greens.at[source, walker, pl.ds(start, size), pl.ds(0, lanes)],
            dst_ref=greens.at[target, walker, pl.ds(start, size), pl.ds(0, lanes)],
            send_sem=ring_send.at[0 if up else 1, step, part],
            recv_sem=ring_recv.at[0 if up else 1, step, part],
            device_id=chip(1 if up else -1),
            device_id_type=MESH,
        )

    def chol_copy(block):
        start = block * BLOCK
        size = min(BLOCK, NOCC - start)
        return pltpu.make_async_copy(
            chol_ref.at[pl.ds(start, size)], raw_chol.at[pl.ds(start, size)], chol_sem.at[block]
        )

    def packing():
        rows = lax.broadcasted_iota(jnp.int32, pack.shape, 0)
        columns = lax.broadcasted_iota(jnp.int32, pack.shape, 1)
        within = lax.rem(columns, 128)
        last = PART + jnp.where(within < PART, 1, 0)
        source = jnp.where(
            columns < 128,
            jnp.where(columns < PART, columns, columns + 128 - PART),
            jnp.where(columns < 256, last, last + 128),
        )
        pack[...] = jnp.where(rows == source, 1.0, 0.0).astype(BF16)

    def clean_pair(pair):
        low = pair * BLOCK
        high = ROWS // 2 + low
        size = min(BLOCK, NOCC - high)
        chol_copy(pair).wait()
        chol_copy(pair + BLOCKS // 2).wait()
        tiles = []
        for start, count in ((low, BLOCK), (high, size)):
            block = pl.ds(start, BLOCK)
            if count < BLOCK:
                chol[pl.ds(start + count, BLOCK - count)] = jnp.zeros(
                    (BLOCK - count, vectors, LANES), BF16
                )
            chol[pl.ds(start, count), :, 0:FULL] = raw_chol[pl.ds(start, count), :, 0:FULL]
            chol[block, :, FULL:LANES] = jnp.zeros((BLOCK, vectors, LANES - FULL), BF16)
            chol[pl.ds(start, count), :, FULL:NVIR] = raw_chol[pl.ds(start, count), :, FULL:NVIR]
            tiles.append(chol[block, :, FULL:LANES].reshape(BLOCK * vectors, LANES - FULL))
        made = jnp.dot(
            jnp.concatenate(tiles, axis=1), pack[...], preferred_element_type=F32
        )
        chol[pl.ds(low, BLOCK), :, FULL:LANES] = (
            made[:, 0:128].astype(BF16).reshape(BLOCK, vectors, LANES - FULL)
        )
        chol[pl.ds(high, BLOCK), :, FULL:LANES] = jnp.zeros((BLOCK, vectors, LANES - FULL), BF16)
        within = lax.rem(lax.broadcasted_iota(jnp.int32, (vectors, 128), 1), PART)
        for third in range(LAST[1]):
            found = [
                (row, first)
                for base, first in ((low, 128), (high, 256))
                for row in range(BLOCK)
                if base + row < NOCC and (base + row) // PART == third
            ]
            if found:
                kept = leftover[third]
                for row, first in found:
                    index = (row + (low if first == 128 else high)) % PART
                    part = made[row * vectors : (row + 1) * vectors, first : first + 128]
                    kept = jnp.where(within == index, part, kept)
                leftover[third] = kept

    def place_leftover():
        lanes = lax.broadcasted_iota(jnp.int32, (vectors, 128), 1)
        for third in range(LAST[1]):
            for column in range(LAST[0]):
                row = SPARE + LAST[1] * column + third
                value = leftover[third]
                if column:
                    value = pltpu.roll(value, PART, 1)
                old = chol[row, :, FULL:LANES].astype(F32)
                chol[row, :, FULL:LANES] = jnp.where(lanes < PART, old, value).astype(BF16)

    def add_block(slots, block):
        rows = pl.ds(pl.multiple_of(block * BLOCK, BLOCK), BLOCK)
        left = chol[rows].reshape(BLOCK * vectors, LANES)
        right = jnp.concatenate(
            [greens[slot, walker, rows, :] for slot in slots for walker in range(2)], axis=0
        )
        total[...] += transposed_dot(left, right)

    def forward(step, part, up, down):
        ring_copy(True, step, part).wait_recv()
        if up:
            ring_copy(True, step + 1, part).start()
        ring_copy(False, step, part).wait_recv()
        if down:
            ring_copy(False, step + 1, part).start()

    def upper_core():
        greet((1, -1), 0)
        for block in range(BLOCKS // 2):
            chol_copy(block).start()
            chol_copy(block + BLOCKS // 2).start()
        own_walker(1)
        pl.semaphore_wait(barrier, 3)
        rows_to_lower().start()
        for part in LAST_UP + LAST_DOWN:
            if part in LAST_DOWN:
                block_to_upper(part).wait_recv()
            ring_copy(True, 1, part).start()
            ring_copy(False, 1, part).start()

        total[...] = jnp.zeros_like(total)
        leftover[...] = jnp.zeros_like(leftover)
        packing()

        @pl.loop(1, chips)
        def _(slot):
            for walker in range(2):
                greens[slot, walker, SENT:ROWS, 0:FULL] = jnp.zeros((ROWS - SENT, FULL), BF16)
                greens[slot, walker, ROWS // 2 : ROWS, FULL:LANES] = jnp.zeros(
                    (ROWS // 2, LANES - FULL), BF16
                )

        greens[0, 0, SENT:ROWS, 0:FULL] = jnp.zeros((ROWS - SENT, FULL), BF16)
        greens[0, 0, ROWS // 2 : ROWS, FULL:LANES] = jnp.zeros((ROWS // 2, LANES - FULL), BF16)

        for step in (1, 2):
            for part in range(len(CHUNKS)):
                forward(step, part, True, True)
                if (step, part) in CLEANED:
                    clean_pair(CLEANED[step, part])
        place_leftover()

        @pl.loop(3, half - 1)
        def _(step):
            pair = lax.div(step - 1, 2)
            second = lax.rem(step - 1, 2)
            slots = (2 * pair - 1, 2 * pair, half + 2 * pair - 1, half + 2 * pair)
            for part in range(len(CHUNKS)):
                forward(step, part, True, True)
                for block in HALF_BLOCKS[part]:
                    add_block(slots, second * (BLOCKS // 2) + block)

            @pl.when(second == 1)
            def _():
                places = (slots[0], slots[1], chips + 1 - 2 * pair, chips - 2 * pair)
                keep_rows(places)
                for place in places:
                    back_copy(place).start()
                    back_copy_lower(place).start()

        step = half - 1
        slots = (half - 3, half - 2, 2 * half - 3, 2 * half - 2)
        for part in range(len(CHUNKS)):
            forward(step, part, part in LAST_UP, part in LAST_DOWN)
            for block in ALL_BLOCKS[part]:
                add_block(slots, block)
        places = (half - 3, half - 2, half + 3, half + 2)
        keep_rows(places)
        for place in places:
            back_copy(place).start()
            back_copy_lower(place).start()

        slots = (half, half - 1, 2 * half - 1, 0)
        for part in range(len(CHUNKS)):
            ring_copy(part in LAST_UP, half, part).wait_recv()
            for block in LAST_BLOCKS[part]:
                add_block(slots, block)
        keep_rows((half, half - 1, half + 1, 0))
        for place in (half, half - 1, half + 1):
            back_copy_lower(place).start()
            back_copy(place).start()
        back_copy_lower(0).start()
        inbox[lax.rem(me, 2), lax.div(me, 2)] = message[0]

        rows_to_lower().wait_send()
        for part in range(len(CHUNKS)):
            ring_copy(True, 1, part).wait_send()
            ring_copy(False, 1, part).wait_send()

        @pl.loop(2, half)
        def _(step):
            for part in range(len(CHUNKS)):
                ring_copy(True, step, part).wait_send()
                ring_copy(False, step, part).wait_send()

        for part in range(len(CHUNKS)):
            ring_copy(part in LAST_UP, half, part).wait_send()
        corr_to_upper().wait_recv()
        inbox_swap(0).wait_recv()
        for offset in range(1, chips):
            back_copy(offset).wait_send()
        for offset in range(1, chips):
            back_wait(offset)
        write_bias(corr_in[1:2, 0:1], inbox[...], peer_inbox[...], True)
        for offset in range(chips):
            back_copy_lower(offset).wait_send()

    up_hops = members // 2
    down_hops = members - 1 - up_hops

    def hop_copy(buffer, send, recv, up, number):
        source = (number - 1) if up else (members - (number - 1)) % members
        target = number if up else members - number
        return pltpu.make_async_remote_copy(
            src_ref=buffer.at[0, source],
            dst_ref=buffer.at[0, target],
            send_sem=send.at[target],
            recv_sem=recv.at[target],
            device_id=chip(STRIDE if up else -STRIDE),
            device_id_type=MESH,
        )

    both_ways = (2, members // 2)

    def shift_of(place, member):
        return -SHIFTS[place] if place == 2 and member >= members // 2 else SHIFTS[place]

    def member_of(place, member):
        return 0 if (place, member) == both_ways else member

    def near_copy(buffer, send, recv, place, member):
        return pltpu.make_async_remote_copy(
            src_ref=buffer.at[0, member_of(place, member)],
            dst_ref=buffer.at[place, member],
            send_sem=send.at[place, member],
            recv_sem=recv.at[place, member],
            device_id=chip(shift_of(place, member)),
            device_id_type=MESH,
        )

    def start_spread(buffer, sems):
        send, recv, send_near, recv_near = sems
        hop_copy(buffer, send, recv, True, 1).start()
        if down_hops:
            hop_copy(buffer, send, recv, False, 1).start()
        for place in (1, 2, 3):
            near_copy(buffer, send_near, recv_near, place, 0).start()
        near_copy(buffer, send_near, recv_near, *both_ways).start()

    def hop_members(number):
        found = [number] if number <= up_hops else []
        return found + ([members - number] if number <= down_hops else [])

    def take_hop(buffer, sems, number):
        send, recv, send_near, recv_near = sems
        if number <= up_hops:
            hop_copy(buffer, send, recv, True, number).wait_recv()
            if number < up_hops:
                hop_copy(buffer, send, recv, True, number + 1).start()
        if number <= down_hops:
            hop_copy(buffer, send, recv, False, number).wait_recv()
            if number < down_hops:
                hop_copy(buffer, send, recv, False, number + 1).start()
        for member in hop_members(number):
            for place in (2, 1, 3):
                if (place, member) != both_ways:
                    near_copy(buffer, send_near, recv_near, place, member).start()

    def take_near(buffer, sems, member):
        for place in (1, 2, 3):
            near_copy(buffer, sems[2], sems[3], place, member).wait_recv()

    def end_spread(buffer, sems):
        send, recv, send_near, recv_near = sems
        for number in range(1, up_hops + 1):
            hop_copy(buffer, send, recv, True, number).wait_send()
        for number in range(1, down_hops + 1):
            hop_copy(buffer, send, recv, False, number).wait_send()
        for member in range(members):
            for place in (1, 2, 3):
                near_copy(buffer, send_near, recv_near, place, member).wait_send()

    def add_determinants(member):
        table = jnp.concatenate([tables[place, member] for place in range(4)], axis=1).astype(F32)
        width = table.shape[1]
        amplitude = table[8:9] + table[9:10] + table[10:11]
        orbital = lax.broadcasted_iota(jnp.int32, (NAO, width), 0).astype(F32)
        particle_hot = jnp.concatenate(
            [
                jnp.where(orbital == table[4 + row : 5 + row], 1.0, 0.0).astype(BF16)
                for row in range(MAXEXC)
            ],
            axis=1,
        )
        picked = jnp.dot(active[:, 0:NAV], particle_hot, preferred_element_type=F32)
        masks = [orbital == table[column : column + 1] for column in range(MAXEXC)]
        pieces = []
        for walker in range(2):
            rows = slice(walker * NAO, (walker + 1) * NAO)
            matrix = []
            for row in range(MAXEXC):
                own = picked[rows, row * width : (row + 1) * width]
                entries = [
                    jnp.sum(jnp.where(masks[column], own, 0.0), axis=0, keepdims=True)
                    for column in range(MAXEXC)
                ]
                entries[row] = jnp.where(table[4 + row : 5 + row] < 0.0, 1.0, entries[row])
                matrix.append(entries)
            ratios, pullback = jax.vjp(minor_determinant, matrix)
            cofactors = pullback(jnp.ones_like(ratios))[0]
            corr_total[walker] += ratios * amplitude
            uppers, lowers = [], []
            for row in range(MAXEXC):
                spread = jnp.zeros((NAO, width), F32)
                for column in range(MAXEXC):
                    spread = jnp.where(masks[column], cofactors[row][column] * amplitude, spread)
                upper = spread.astype(BF16)
                uppers.append(upper)
                lowers.append((spread - upper.astype(F32)).astype(BF16))
            pieces += [jnp.concatenate(uppers, axis=1), jnp.concatenate(lowers, axis=1)]
        grad_total[:, 0:NAV] += transposed_dot(jnp.concatenate(pieces, axis=0), particle_hot)

    def finish_gradient():
        for walker in range(2):
            start = 2 * walker * NAO
            whole = grad_total[start : start + NAO, :] + grad_total[start + NAO : start + 2 * NAO, :]
            packed = whole[0 : NAO // 2] + pltpu.roll(whole[NAO // 2 : NAO], NAV, 1)
            gradients[0, 0, walker] = packed.astype(BF16)

    def add_active(member):
        lanes = lax.broadcasted_iota(jnp.int32, (NAO // 2, 128), 1)
        unpacked = []
        for place in range(4):
            for walker in range(2):
                packed = gradients[place, member, walker].astype(F32)
                unpacked.append(
                    (
                        jnp.where(lanes < NAV, packed, 0.0).astype(BF16),
                        jnp.where(lanes < NAV, pltpu.roll(packed, NAV, 1), 0.0).astype(BF16),
                    )
                )
        for block in range(NAO // BLOCK):
            left = active_chol[pl.ds(block * BLOCK, BLOCK)].reshape(BLOCK * vectors, 128)
            side, inner = divmod(block * BLOCK, NAO // 2)
            right = jnp.concatenate(
                [halves[side][inner : inner + BLOCK] for halves in unpacked], axis=0
            )
            total[...] += transposed_dot(left, right)
        places = [(shift_of(place, member) + STRIDE * member_of(place, member)) % chips for place in range(4)]
        keep_rows(places)
        for place in places:
            if place:
                back_copy(place).start()

    table_sems = (table_send, table_recv, table_send_near, table_recv_near)
    grad_sems = (grad_send, grad_recv, grad_send_near, grad_recv_near)

    def lower_core():
        chol_part = pltpu.make_async_copy(
            chol_ref.at[pl.ds(NOCC - NAO, NAO), :, pl.ds(0, 128)], active_chol, chol_sem.at[0]
        )
        chol_part.start()
        greet((1, -1), 1)
        own_walker(0)
        pl.semaphore_wait(barrier, 3)
        for part in LAST_DOWN:
            block_to_upper(part).start()
        for offset in (1, -1):
            pl.semaphore_signal(near_sem, inc=1, device_id=chip(offset), device_id_type=MESH)

        order = order_ref[...]
        live = lax.broadcasted_iota(jnp.int32, (MAXEXC, order.shape[1]), 0) < order
        table_build[...] = jnp.zeros_like(table_build)
        table_build[0:4, :] = jnp.where(live, hole_ref[...], -1).astype(F32)
        table_build[4:8, :] = jnp.where(live, particle_ref[...], -1).astype(F32)
        amp = amp_ref[...]
        high = amp.astype(BF16).astype(F32)
        middle = (amp - high).astype(BF16).astype(F32)
        table_build[8:9, :] = high
        table_build[9:10, :] = middle
        table_build[10:11, :] = amp - high - middle
        tables[0, 0] = table_build[...].astype(BF16)

        pl.semaphore_wait(near_sem, 2)
        for offset in (2, -2):
            pl.semaphore_signal(far_sem, inc=1, device_id=chip(offset), device_id_type=MESH)
        pl.semaphore_wait(far_sem, 2)
        start_spread(tables, table_sems)

        total[...] = jnp.zeros_like(total)
        grad_total[...] = jnp.zeros_like(grad_total)
        corr_total[...] = jnp.zeros_like(corr_total)
        shift_rows = lax.broadcasted_iota(jnp.int32, (NAO, ROWS // 2), 0)
        shift_columns = lax.broadcasted_iota(jnp.int32, (NAO, ROWS // 2), 1)
        offset = NOCC - NAO - ROWS // 2
        shift = (shift_columns == shift_rows + offset).astype(F32).astype(BF16)
        active[0:NAO, :] = jnp.dot(
            shift, greens[0, 0, ROWS // 2 : ROWS, 0:128], preferred_element_type=F32
        ).astype(BF16)
        rows_to_lower().wait_recv()
        active[NAO : 2 * NAO, :] = jnp.dot(
            shift, peer_rows[...], preferred_element_type=F32
        ).astype(BF16)

        late = [0]
        for number in range(1, up_hops + 1):
            take_hop(tables, table_sems, number)
            for member in late:
                take_near(tables, table_sems, member)
                add_determinants(member)
            late = hop_members(number)
        for member in late:
            take_near(tables, table_sems, member)
            add_determinants(member)
        finish_gradient()
        start_spread(gradients, grad_sems)

        for walker in range(2):
            corr_out[walker : walker + 1, :] = jnp.broadcast_to(
                1.0 + jnp.sum(corr_total[walker], axis=1, keepdims=True), (1, 128)
            )
        chol_part.wait()

        late = [0]
        for number in range(1, up_hops + 1):
            take_hop(gradients, grad_sems, number)
            if number == 1:
                corr_to_upper().start()
            for member in late:
                take_near(gradients, grad_sems, member)
                add_active(member)
            late = hop_members(number)
        for member in late:
            take_near(gradients, grad_sems, member)
            add_active(member)
        inbox[lax.rem(me, 2), lax.div(me, 2)] = message[0]

        end_spread(tables, table_sems)
        end_spread(gradients, grad_sems)
        for part in LAST_DOWN:
            block_to_upper(part).wait_send()
        corr_to_upper().wait_send()
        for offset in range(1, chips):
            back_copy(offset).wait_send()
        for offset in range(1, chips):
            back_wait(offset)
        inbox_swap(1).start()
        inbox_swap(1).wait_send()
        for offset in range(chips):
            back_wait_lower(offset)
        write_bias(corr_out[0:1, 0:1], peer_inbox[...], inbox[...], False)

    @pl.when(core == 1)
    def _():
        upper_core()

    @pl.when(core == 0)
    def _():
        lower_core()


def shards(greens, chol_vectors, hole_orbitals, particle_orbitals, excitation_order, amplitudes):
    chips = lax.axis_size("det")
    vectors = chol_vectors.shape[0]
    dets = hole_orbitals.shape[0]
    members = chips // STRIDE
    half = chips // 2
    dma = pltpu.SemaphoreType.DMA
    vmem = pl.BlockSpec(memory_space=pltpu.VMEM)
    corr, bias = pl.pallas_call(
        functools.partial(kernel, chips),
        out_shape=(
            jax.ShapeDtypeStruct((1, 128), F32),
            jax.ShapeDtypeStruct((chips * vectors // 128, 128), F32),
        ),
        in_specs=[vmem, pl.BlockSpec(memory_space=pl.ANY), vmem, vmem, vmem, vmem],
        out_specs=(vmem, vmem),
        scratch_shapes=[
            pltpu.VMEM((NOCC, vectors, NVIR), BF16),
            pltpu.VMEM((ROWS, vectors, LANES), BF16),
            pltpu.VMEM((NAO, vectors, 128), BF16),
            pltpu.VMEM((chips, 2, ROWS, LANES), BF16),
            pltpu.VMEM((BLOCK * vectors, BATCH * BLOCK), F32),
            pltpu.VMEM((4, members, 16, dets), BF16),
            pltpu.VMEM((4, members, 2, NAO // 2, 128), BF16),
            pltpu.VMEM((16, dets), F32),
            pltpu.VMEM((ROWS // 2, 128), BF16),
            pltpu.VMEM((2 * NAO, 128), BF16),
            pltpu.VMEM((4 * NAO, 128), F32),
            pltpu.VMEM((2, 1, 4 * dets), F32),
            pltpu.VMEM((chips, 1, 128), F32),
            pltpu.VMEM((2, half, 1, 128), F32),
            pltpu.VMEM((2, half, 1, 128), F32),
            pltpu.VMEM((8, 128), F32),
            pltpu.VMEM((8, 128), F32),
            pltpu.VMEM((256, 384), BF16),
            pltpu.VMEM((LAST[1], vectors, 128), F32),
            dma((BLOCKS,)),
            dma((4 + len(CHUNKS) // 2,)),
            dma((4 + len(CHUNKS) // 2,)),
            dma((2, half + 1, len(CHUNKS))),
            dma((2, half + 1, len(CHUNKS))),
            dma((members,)),
            dma((members,)),
            dma((4, members)),
            dma((4, members)),
            dma((members,)),
            dma((members,)),
            dma((4, members)),
            dma((4, members)),
            dma((chips,)),
            dma((chips,)),
            dma((chips,)),
            dma((chips,)),
            pltpu.SemaphoreType.REGULAR,
            pltpu.SemaphoreType.REGULAR,
        ],
        compiler_params=pltpu.CompilerParams(
            collective_id=0, has_side_effects=True, vmem_limit_bytes=56 * 1024 * 1024
        ),
        name="walker_ring",
    )(
        jnp.transpose(greens, (0, 2, 1)).reshape(NOCC, NVIR),
        jnp.transpose(chol_vectors, (2, 0, 1)),
        jnp.transpose(hole_orbitals),
        jnp.transpose(particle_orbitals),
        excitation_order.reshape(1, dets),
        amplitudes.reshape(1, dets),
    )
    return (corr[0, 0:1], bias.reshape(1, chips * vectors))


def solution(mesh):
    placed = (
        P(("grp", "det", "wlk"), None, None),
        P(("grp", "det"), None, None),
        P(("grp", "det"), None),
        P(("grp", "det"), None),
        P(("grp", "det")),
        P(("grp", "det")),
    )
    return jax.shard_map(
        shards,
        mesh=mesh,
        in_specs=placed,
        out_specs=(P(("grp", "det", "wlk")), P(("grp", "det", "wlk"), None)),
        check_vma=False,
    )
```
